256 devices in a mesh: dp: 32 (over z, x), parity: 8 (over y, core).
Axes of the slice: x: 4, y: 4, z: 8, core: 2. Of those that a mesh axis runs over, the one named last changes fastest.
Arguments:
- first_moment: float32 [131072, 512], P(('dp', 'parity')), may hold values from -6 to 6
- second_moment: float32 [131072, 512], P(('dp', 'parity')), may hold values from 0.01 to 4
- new_owner: int32 [131072, 1], P(('dp', 'parity')), may hold values from 0 to 31; in each aligned block of 512 rows (0 to 511, 512 to 1023, ...) at most 20 rows name the same one
- code_index: int32 [2, 8], replicated, may hold values from 0 to 7
Outputs:
- new_first: float32 [163840, 512], P(('dp', 'parity'))
- new_second: float32 [163840, 512], P(('dp', 'parity'))
- parity: float32 [20480, 2048], P(('dp', 'parity'))
- loads: int32 [32, 8], P('dp', 'parity')
The draws below stay inside these ranges and needn't reach their ends.
Inputs may be any that keep to these rules, and one draw needn't show every extreme that they name: `new_owner`: in the rows of one device (aligned blocks of 512 rows) no owner is named more than 20 times, a bound that some owner reaches in some blocks.
All inputs are finite; a program needn't handle non-finite values.
Results may differ from the reference program's by a relative error of at most 0.0003.
Values sent between devices are 32-bit elements; how exact they have to be, the bound alone decides.
A program may use at most 64 MiB of HBM per device.

```python
import math
import jax
import jax.numpy as jnp
import numpy as np
from jax import lax

BLOCK = 512
PARITY_UNITS = 2
BLK_DEV = 512
MOST = 20
CAP = 640
BLOCKS = 131072
N_DP = 32
N_PARITY = 8


def place_ends(drawn, key, smallest, top_value):
    spot = [jax.random.randint(jax.random.fold_in(key, axis), (), 0, length) for axis, length in enumerate(drawn.shape)]
    widest = drawn.shape.index(max(drawn.shape))
    beside = spot[:widest] + [(spot[widest] + 1) % drawn.shape[widest]] + spot[widest + 1:]
    return drawn.at[tuple(spot)].set(smallest).at[tuple(beside)].set(top_value)


def block_levels(own_key, extent, split, low, high):
    level, own = 1.0, jax.random.fold_in(own_key, 6)
    for position, parts in split:
        draws = jnp.exp(jax.random.uniform(jax.random.fold_in(own, position), (parts,), jnp.float32, low / len(split), high / len(split)))
        level = level * jnp.repeat(draws, extent[position] // parts).reshape([-1 if axis == position else 1 for axis in range(len(extent))])
    return level


def shared_out(own_key, own, number, rows, number_of, top, bound, slope):
    sequence = jax.random.permutation(own_key, number_of)
    crowded, ordinary = shares(number_of, rows * top, bound, slope, True), shares(number_of, rows * top, bound, slope, False)
    places = jnp.arange(number_of)

    def named(lengths, offset_by):
        used = int((lengths > 0).sum())
        fixed = max(1, used // 4)
        passed = fixed + (places - fixed + offset_by * (used - fixed)) % max(1, number_of - fixed)
        return jnp.zeros((number_of,), jnp.int32).at[sequence[jnp.where(places < fixed, places, passed)]].set(jnp.asarray(lengths, jnp.int32))

    lengths = jnp.where(number % 4 == 0, named(crowded, number // 4), named(ordinary, number - number // 4 - 1))
    mixed = jax.random.permutation(jax.random.fold_in(own, 3), number_of)
    source_of, taker = mixed[0:number_of // 2 * 2:2], mixed[1:number_of // 2 * 2:2]
    slack = jnp.minimum(lengths[source_of] - 1, bound - lengths[taker]) // 2
    slack = jnp.where((source_of == sequence[0]) | (taker == sequence[0]) | (lengths[taker] == 0), 0, jnp.maximum(slack, 0))
    passed = jax.random.randint(jax.random.fold_in(own, 4), (number_of // 2,), 0, 1 << 20) % (slack + 1)
    lengths = lengths.at[source_of].add(-passed).at[taker].add(passed)
    items = jnp.searchsorted(jnp.cumsum(lengths), jnp.arange(rows * top), side="right").astype(jnp.int32)
    grid = items.reshape(top, rows).T
    grid = grid[jax.random.permutation(jax.random.fold_in(own, 1), rows)]
    offset_by = jax.random.randint(jax.random.fold_in(own, 2), (rows, 1), 0, top)
    return jnp.take_along_axis(grid, (jnp.arange(top)[None, :] + offset_by) % top, axis=1)


def shares(count, total, bound, skew, full):
    weights = [(1 << 20) // math.isqrt(standing ** skew) + 1 for standing in range(1, count + 1)]
    largest = bound if full else min(bound, max(-(-total // count), total * weights[0] // sum(weights)))
    least = 1 if total - largest >= count - 1 else 0
    counts, rest = [largest] + [least] * (count - 1), total - largest - least * (count - 1)
    while rest > 0:
        candidates = [i for i in range(1, count) if counts[i] < largest] or [i for i in range(1, count) if counts[i] < bound]
        mass, budget = sum([weights[i] for i in candidates]), rest
        for i in candidates:
            addition = min(bound - counts[i], max(1, budget * weights[i] // mass), rest)
            counts[i] = counts[i] + addition
            rest = rest - addition
    return np.array(counts)


def bell_draw(stream_key, extent, scale, most, pieces=(), kind=jnp.bfloat16):
    gain = block_levels(stream_key, extent, pieces, -0.22, 0.18) if pieces else 1.0
    result = jax.random.normal(stream_key, extent, jnp.float32) * scale * gain
    return jnp.minimum(jnp.maximum(result, -most), most).astype(kind)


def setup_inputs(seed: int = 0) -> dict:
    keys = jax.random.split(jax.random.key(seed), 5)
    first_moment = bell_draw(keys[0], (BLOCKS, BLOCK), 1.0, 6.0, ((0, 256),), jnp.float32)
    second_moment = jnp.clip(jnp.exp(math.log(4.0) - 5.9914646 * jax.random.uniform(keys[1], (BLOCKS, BLOCK), jnp.float32) ** block_levels(keys[1], (BLOCKS, BLOCK), ((0, 256),), -0.2, 0.2)), 0.01, 4.0)
    new_owner_keys = jax.random.split(jax.random.fold_in(keys[2], 1), BLOCKS // BLK_DEV)
    new_owner_turns = jax.random.permutation(jax.random.fold_in(keys[2], 3), BLOCKS // BLK_DEV)
    new_owner = jax.vmap(lambda own, number: shared_out(jax.random.fold_in(keys[2], 2), own, number, BLK_DEV, N_DP, 1, MOST, 2))(new_owner_keys, new_owner_turns).reshape((BLOCKS, 1))
    code_index = place_ends(jax.random.randint(keys[3], (PARITY_UNITS, N_PARITY), 0, 8), jax.random.fold_in(keys[3], 1), 0, 7).astype(jnp.int32)
    return {"first_moment": first_moment, "second_moment": second_moment, "new_owner": new_owner, "code_index": code_index}


def reference(first_moment, second_moment, new_owner, code_index):
    owner = new_owner.reshape(N_DP, N_PARITY, BLK_DEV).astype(jnp.int32)
    owners = jnp.arange(N_DP, dtype=jnp.int32)
    onehot = (owner[:, :, :, None] == owners[None, None, None, :]).astype(jnp.int32)
    before = (jnp.cumsum(onehot, axis=2).astype(jnp.int32) - onehot).astype(jnp.int32)
    rank = jnp.sum(before * onehot, axis=3).astype(jnp.int32)
    source = jnp.arange(N_DP, dtype=jnp.int32)[:, None, None]
    column = jnp.arange(N_PARITY, dtype=jnp.int32)[None, :, None]
    target = ((owner * N_PARITY + column) * CAP + source * MOST + rank).reshape(-1).astype(jnp.int32)
    new_first = jnp.zeros((N_DP * N_PARITY * CAP, BLOCK), jnp.float32).at[target].set(first_moment)
    new_second = jnp.zeros((N_DP * N_PARITY * CAP, BLOCK), jnp.float32).at[target].set(second_moment)
    loads = jnp.transpose(jnp.sum(onehot, axis=(0, 2)).astype(jnp.int32))
    coef = code_index.astype(jnp.float32) * 0.25
    stacked = jnp.concatenate([new_first, new_second], axis=1).reshape(N_DP, N_PARITY, CAP, 2 * BLOCK)
    parity = jnp.einsum("rp,dpsc->dsrc", coef, stacked, precision=lax.Precision.HIGHEST)
    parity = parity.reshape(N_DP * CAP, PARITY_UNITS * 2 * BLOCK)
    return new_first, new_second, parity, loads
```

```python
import functools

import jax
import jax.numpy as jnp
from jax import lax
from jax.experimental import pallas as pl
from jax.experimental.pallas import tpu as pltpu
from jax.sharding import PartitionSpec as P

MESH = pl.DeviceIdType.MESH
NZ, NX = 8, 4
N_DP = NZ * NX
N_PAR = 8
ROOM = 20
BLK = 512
WIDTH = 512
PAIR = 2 * ROOM
GROUP = 8
LANE = 32


def exchange(first_hbm, second_hbm, owner_ref, code_ref,
             new_first, new_second, parity, loads,
             x_first, x_second, parts, send, recv, share, cnt_send, cnt_recv,
             in_sem, send_sem, recv_sem, cs_sem, cr_sem, ps_sem, pr_sem):
    me = lax.axis_index("dp")
    col = lax.axis_index("parity")
    z = lax.div(me, NX)
    x = lax.rem(me, NX)

    loads_in = [
        pltpu.make_async_copy(first_hbm, x_first, in_sem.at[0]),
        pltpu.make_async_copy(second_hbm, x_second, in_sem.at[1]),
    ]
    for c in loads_in:
        c.start()

    barrier = pltpu.get_barrier_semaphore()
    for k in range(1, N_DP):
        pl.semaphore_signal(barrier, inc=1, device_id={"dp": lax.rem(me + k, N_DP)}, device_id_type=MESH)
    for k in range(1, N_PAR):
        pl.semaphore_signal(barrier, inc=1, device_id={"parity": lax.rem(col + k, N_PAR)}, device_id_type=MESH)

    owner = owner_ref[...]
    onehot = (lax.broadcasted_iota(jnp.int32, (N_DP, BLK), 0) == owner).astype(jnp.float32)
    earlier = lax.broadcasted_iota(jnp.int32, (BLK, BLK), 0) < lax.broadcasted_iota(jnp.int32, (BLK, BLK), 1)
    before = jnp.dot(onehot.astype(jnp.bfloat16), earlier.astype(jnp.float32).astype(jnp.bfloat16),
                     preferred_element_type=jnp.float32)
    rank = jnp.sum(before * onehot, axis=0, keepdims=True)
    key = owner.astype(jnp.float32) * LANE + rank
    counts = jnp.sum(onehot, axis=1, keepdims=True).astype(jnp.int32)
    counts = jnp.broadcast_to(counts, (N_DP, 128))
    for d in range(N_DP):
        cnt_send[d] = counts[d:d + 1]

    for m, (c, src) in enumerate(zip(loads_in, (x_first, x_second))):
        c.wait()
        whole = src[...]
        high = whole.astype(jnp.bfloat16)
        rest = whole - high.astype(jnp.float32)
        mid = rest.astype(jnp.bfloat16)
        parts[3 * m] = high
        parts[3 * m + 1] = mid
        parts[3 * m + 2] = (rest - mid.astype(jnp.float32)).astype(jnp.bfloat16)

    rows = 24
    shape = (GROUP, rows, BLK)
    slot = (lax.broadcasted_iota(jnp.int32, shape, 0) * LANE + lax.broadcasted_iota(jnp.int32, shape, 1))
    slot = slot.reshape(GROUP * rows, BLK).astype(jnp.float32)

    def build(g, carry):
        base = key - (g * (GROUP * LANE)).astype(jnp.float32)
        chosen = []
        for m in range(2):
            pick = jnp.where(slot == base + 4.0 * m, 1.0, 0.0).astype(jnp.bfloat16)
            out = jnp.dot(pick, parts[3 * m], preferred_element_type=jnp.float32)
            out = out + jnp.dot(pick, parts[3 * m + 1], preferred_element_type=jnp.float32)
            out = out + jnp.dot(pick, parts[3 * m + 2], preferred_element_type=jnp.float32)
            chosen.append(out.reshape(GROUP, rows, WIDTH))
        a, b = chosen
        for o in range(GROUP):
            d = g * GROUP + o
            send[d, 0:16] = a[o, 0:16]
            send[d, 16:24] = a[o, 16:24] + b[o, 0:8]
            send[d, 24:40] = b[o, 8:24]
        return carry

    lax.fori_loop(0, N_DP // GROUP, build, 0)
    pl.semaphore_wait(barrier, N_DP - 1 + N_PAR - 1)

    def step(i):
        i = lax.rem(i + col, NZ)
        half = lax.div(i, 2)
        return jnp.where(lax.rem(i, 2) == 0, half, NZ - 1 - half)

    def ids(i, dx):
        dz = step(i)
        to = lax.rem(z + dz, NZ) * NX + lax.rem(x + dx, NX)
        source_z = lax.rem(z - dz + NZ, NZ)
        source_x = lax.rem(x - dx + NX, NX)
        return dz, dz * NX + dx, to, source_z, source_x

    def block_copy(to, k, landing):
        return pltpu.make_async_remote_copy(
            src_ref=send.at[to], dst_ref=recv.at[landing], send_sem=send_sem.at[k], recv_sem=recv_sem.at[k],
            device_id={"dp": to}, device_id_type=MESH)

    def count_copy(to, k, landing):
        return pltpu.make_async_remote_copy(
            src_ref=cnt_send.at[to], dst_ref=cnt_recv.at[landing], send_sem=cs_sem.at[k], recv_sem=cr_sem.at[k],
            device_id={"dp": to}, device_id_type=MESH)

    def share_copy(source, source_x, target, from_col):
        return pltpu.make_async_remote_copy(
            src_ref=recv.at[source], dst_ref=share.at[from_col * NX + source_x],
            send_sem=ps_sem.at[source], recv_sem=pr_sem.at[from_col * NX + source_x],
            device_id={"parity": target}, device_id_type=MESH)

    def issue(i, carry):
        for dx in range(NX):
            dz, k, to, _, _ = ids(i, dx)

            @pl.when(k != 0)
            def _():
                block_copy(to, k, me).start()
                count_copy(to, k, me).start()
        return carry

    lax.fori_loop(0, NZ, issue, 0)
    recv[me] = send[me]
    cnt_recv[me] = cnt_send[me]

    def arrive(i, carry):
        for dx in range(NX):
            dz, k, to, sz, sx = ids(i, dx)
            source = sz * NX + sx

            @pl.when(k != 0)
            def _():
                block_copy(to, k, source).wait_recv()

            @pl.when(sz != col)
            def _():
                share_copy(source, sx, sz, col).start()

            @pl.when(sz == col)
            def _():
                share[col * NX + sx] = recv[source]
        for h in range(NX // 2):
            one, two = sz * NX + 2 * h, sz * NX + 2 * h + 1
            at = pl.ds(pl.multiple_of((sz * (NX // 2) + h) * PAIR, 8), PAIR)
            new_first[at] = jnp.concatenate([recv[one, 0:ROOM], recv[two, 0:ROOM]], axis=0)
            new_second[at] = jnp.concatenate([recv[one, ROOM:PAIR], recv[two, ROOM:PAIR]], axis=0)
        return carry

    lax.fori_loop(0, NZ, arrive, 0)

    def counted(i, carry):
        for dx in range(NX):
            _, k, to, sz, sx = ids(i, dx)

            @pl.when(k != 0)
            def _():
                count_copy(to, k, sz * NX + sx).wait()
                block_copy(to, k, sz * NX + sx).wait_send()
        return carry

    lax.fori_loop(0, NZ, counted, 0)
    total = cnt_recv[0]
    for d in range(1, N_DP):
        total = total + cnt_recv[d]
    loads[...] = total

    def shared(other, carry):
        @pl.when(other != col)
        def _():
            for sx in range(NX):
                share_copy(other * NX + sx, sx, other, other).wait_recv()
                share_copy(other * NX + sx, sx, other, col).wait_send()
        return carry

    lax.fori_loop(0, N_PAR, shared, 0)
    coef = [[code_ref[r, p].astype(jnp.float32) * 0.25 for p in range(N_PAR)] for r in range(2)]
    for h in range(NX // 2):
        sums = [[None, None], [None, None]]
        for r in range(2):
            for o in range(2):
                acc = coef[r][0] * share[2 * h + o]
                for p in range(1, N_PAR):
                    acc = acc + coef[r][p] * share[p * NX + 2 * h + o]
                sums[r][o] = acc
        for r in range(2):
            one, two = sums[r]
            at = slice(h * PAIR, (h + 1) * PAIR)
            parity[at, (2 * r) * WIDTH:(2 * r + 1) * WIDTH] = jnp.concatenate([one[0:ROOM], two[0:ROOM]], axis=0)
            parity[at, (2 * r + 1) * WIDTH:(2 * r + 2) * WIDTH] = jnp.concatenate([one[ROOM:PAIR], two[ROOM:PAIR]], axis=0)


def put_out(nf, ns, par, cnt, nf_out, ns_out, par_out, cnt_out, sem):
    copies = [
        pltpu.make_async_copy(nf, nf_out, sem.at[0]),
        pltpu.make_async_copy(ns, ns_out, sem.at[1]),
        pltpu.make_async_copy(par, par_out, sem.at[2]),
    ]
    for c in copies:
        c.start()
    cnt_out[...] = cnt[0:1, 0:1]
    for c in copies:
        c.wait()


def body(first_moment, second_moment, new_owner, code_index):
    f32, i32 = jnp.float32, jnp.int32
    capacity = N_DP * ROOM
    vmem = pl.BlockSpec(memory_space=pltpu.VMEM)
    anywhere = pl.BlockSpec(memory_space=pl.ANY)
    dma = pltpu.SemaphoreType.DMA
    held = pl.pallas_call(
        exchange,
        out_shape=(jax.ShapeDtypeStruct((capacity, WIDTH), f32), jax.ShapeDtypeStruct((capacity, WIDTH), f32),
                   jax.ShapeDtypeStruct((capacity // N_PAR, 4 * WIDTH), f32), jax.ShapeDtypeStruct((1, 128), i32)),
        in_specs=[anywhere, anywhere, vmem, pl.BlockSpec(memory_space=pltpu.SMEM)],
        out_specs=(vmem, vmem, vmem, vmem),
        scratch_shapes=[
            pltpu.VMEM((BLK, WIDTH), f32), pltpu.VMEM((BLK, WIDTH), f32), pltpu.VMEM((6, BLK, WIDTH), jnp.bfloat16),
            pltpu.VMEM((N_DP, PAIR, WIDTH), f32), pltpu.VMEM((N_DP, PAIR, WIDTH), f32),
            pltpu.VMEM((N_PAR * NX, PAIR, WIDTH), f32),
            pltpu.VMEM((N_DP, 1, 128), i32), pltpu.VMEM((N_DP, 1, 128), i32),
            dma((2,)), dma((N_DP,)), dma((N_DP,)), dma((N_DP,)), dma((N_DP,)), dma((N_DP,)), dma((N_DP,)),
        ],
        compiler_params=pltpu.CompilerParams(collective_id=0, has_side_effects=True, vmem_limit_bytes=32 * 2**20),
    )(first_moment, second_moment, new_owner.reshape(1, BLK), code_index)
    return pl.pallas_call(
        put_out,
        out_shape=(jax.ShapeDtypeStruct((capacity, WIDTH), f32), jax.ShapeDtypeStruct((capacity, WIDTH), f32),
                   jax.ShapeDtypeStruct((capacity // N_PAR, 4 * WIDTH), f32), jax.ShapeDtypeStruct((1, 1), i32)),
        in_specs=[vmem, vmem, vmem, vmem],
        out_specs=(anywhere, anywhere, anywhere, vmem),
        scratch_shapes=[dma((3,))],
        compiler_params=pltpu.CompilerParams(vmem_limit_bytes=16 * 2**20),
    )(*held)


def solution(mesh):
    rows = P(("dp", "parity"), None)
    return jax.shard_map(body, mesh=mesh, in_specs=(rows, rows, rows, P()),
                         out_specs=(rows, rows, rows, P("dp", "parity")), check_vma=False)
```

```python
import functools

import jax
import jax.numpy as jnp
from jax import lax
from jax.experimental import pallas as pl
from jax.experimental.pallas import tpu as pltpu
from jax.sharding import PartitionSpec as P

MESH = pl.DeviceIdType.MESH
NZ, NX = 8, 4
N_DP = NZ * NX
N_PAR = 8
ROOM = 20
BLK = 512
WIDTH = 512
PAIR = 2 * ROOM
GROUP = 8
PIECES = 4
LANE = 32


def by_class(classes):
    steps = [(0, dx) for dx in range(1, NX)]
    for c in classes:
        for dx in range(NX):
            steps += [(c, dx)] if 2 * c == NZ else [(c, dx), (NZ - c, dx)]
    return [dz * NX + dx for dz, dx in steps]


ISSUE = (by_class((1, 2, 3, 4)), by_class((3, 4, 1, 2)))
WAIT = ISSUE
DONE = tuple([max(w.index(k) for k in range(dz * NX, dz * NX + NX) if k) for dz in range(NZ)] for w in WAIT)
PLANES = tuple(sorted(range(NZ), key=done.__getitem__) for done in DONE)
PLACED = [max(done[planes[j]] for done, planes in zip(DONE, PLANES)) for j in range(NZ)]


def exchange(first_hbm, second_hbm, owner_hbm, code_hbm,
             new_first, new_second, parity, loads,
             owner_ref, code_ref, x_first, x_second, parts, send, recv, share, sums, cnt_send, cnt_recv,
             in_sem, send_sem, recv_sem, cs_sem, cr_sem, ps_sem, pr_sem):
    me = lax.axis_index("dp")
    col = lax.axis_index("parity")
    z = lax.div(me, NX)
    x = lax.rem(me, NX)

    loads_in = [
        pltpu.make_async_copy(first_hbm, x_first, in_sem.at[0]),
        pltpu.make_async_copy(second_hbm, x_second, in_sem.at[1]),
    ]
    small_in = [
        pltpu.make_async_copy(owner_hbm, owner_ref, in_sem.at[2]),
        pltpu.make_async_copy(code_hbm, code_ref, in_sem.at[3]),
    ]
    for c in small_in + loads_in:
        c.start()

    barrier = pltpu.get_barrier_semaphore()
    for k in range(1, N_DP):
        pl.semaphore_signal(barrier, inc=1, device_id={"dp": lax.rem(me + k, N_DP)}, device_id_type=MESH)
    for k in range(1, N_PAR):
        pl.semaphore_signal(barrier, inc=1, device_id={"parity": lax.rem(col + k, N_PAR)}, device_id_type=MESH)

    for c in small_in:
        c.wait()
    owner = owner_ref[...]
    onehot = (lax.broadcasted_iota(jnp.int32, (N_DP, BLK), 0) == owner).astype(jnp.float32)
    earlier = lax.broadcasted_iota(jnp.int32, (BLK, BLK), 0) < lax.broadcasted_iota(jnp.int32, (BLK, BLK), 1)
    before = jnp.dot(onehot.astype(jnp.bfloat16), earlier.astype(jnp.float32).astype(jnp.bfloat16),
                     preferred_element_type=jnp.float32)
    rank = jnp.sum(before * onehot, axis=0, keepdims=True)
    key = owner.astype(jnp.float32) * LANE + rank
    counts = jnp.sum(onehot, axis=1, keepdims=True).astype(jnp.int32)
    counts = jnp.broadcast_to(counts, (N_DP, 128))
    for d in range(N_DP):
        cnt_send[d] = counts[d:d + 1]

    for m, (c, src) in enumerate(zip(loads_in, (x_first, x_second))):
        c.wait()
        whole = src[...]
        high = whole.astype(jnp.bfloat16)
        rest = whole - high.astype(jnp.float32)
        mid = rest.astype(jnp.bfloat16)
        parts[3 * m] = high
        parts[3 * m + 1] = mid
        parts[3 * m + 2] = (rest - mid.astype(jnp.float32)).astype(jnp.bfloat16)

    rows = 24
    shape = (GROUP, rows, BLK)
    slot = (lax.broadcasted_iota(jnp.int32, shape, 0) * LANE + lax.broadcasted_iota(jnp.int32, shape, 1))
    slot = slot.reshape(GROUP * rows, BLK).astype(jnp.float32)

    def build(g, carry):
        base = key - (g * (GROUP * LANE)).astype(jnp.float32)
        chosen = []
        for m in range(2):
            pick = jnp.where(slot == base + 4.0 * m, 1.0, 0.0).astype(jnp.bfloat16)
            out = jnp.dot(pick, parts[3 * m], preferred_element_type=jnp.float32)
            out = out + jnp.dot(pick, parts[3 * m + 1], preferred_element_type=jnp.float32)
            out = out + jnp.dot(pick, parts[3 * m + 2], preferred_element_type=jnp.float32)
            chosen.append(out.reshape(GROUP, rows, WIDTH))
        a, b = chosen
        for o in range(GROUP):
            d = g * GROUP + o
            send[d, 0:16] = a[o, 0:16]
            send[d, 16:24] = a[o, 16:24] + b[o, 0:8]
            send[d, 24:40] = b[o, 8:24]
        return carry

    with jax.named_scope('build'):
        lax.fori_loop(0, N_DP // GROUP, build, 0)
    with jax.named_scope('barrier'):
        pl.semaphore_wait(barrier, N_DP - 1 + N_PAR - 1)

    core = lax.rem(col, 2)

    def ids(k):
        dz, dx = lax.div(k, NX), lax.rem(k, NX)
        to = lax.rem(z + dz, NZ) * NX + lax.rem(x + dx, NX)
        source_z = lax.rem(z - dz + NZ, NZ)
        source_x = lax.rem(x - dx + NX, NX)
        return to, source_z, source_x

    def pick(table, i):
        return jnp.where(core == 0, table[0][i], table[1][i])

    def block_copy(to, k, landing):
        return pltpu.make_async_remote_copy(
            src_ref=send.at[to], dst_ref=recv.at[landing], send_sem=send_sem, recv_sem=recv_sem.at[k],
            device_id={"dp": to}, device_id_type=MESH)

    def count_copy(to, landing):
        return pltpu.make_async_remote_copy(
            src_ref=cnt_send.at[to], dst_ref=cnt_recv.at[landing], send_sem=cs_sem, recv_sem=cr_sem,
            device_id={"dp": to}, device_id_type=MESH)

    def share_copy(source, source_x, target, from_col):
        return pltpu.make_async_remote_copy(
            src_ref=recv.at[source], dst_ref=share.at[from_col * NX + source_x],
            send_sem=ps_sem, recv_sem=pr_sem.at[from_col * NX + source_x],
            device_id={"parity": target}, device_id_type=MESH)

    with jax.named_scope('issue'):
        for i in range(N_DP - 1):
            k = pick(ISSUE, i)
            to, _, _ = ids(k)
            block_copy(to, k, me).start()
            count_copy(to, me).start()
    recv[me] = send[me]
    cnt_recv[me] = cnt_send[me]

    def place(sz):
        for h in range(NX // 2):
            one, two = sz * NX + 2 * h, sz * NX + 2 * h + 1
            at = pl.ds(pl.multiple_of((sz * (NX // 2) + h) * PAIR, 8), PAIR)
            new_first[at] = jnp.concatenate([recv[one, 0:ROOM], recv[two, 0:ROOM]], axis=0)
            new_second[at] = jnp.concatenate([recv[one, ROOM:PAIR], recv[two, ROOM:PAIR]], axis=0)

    def forward(source, sz, sx):
        @pl.when(sz != col)
        def _():
            share_copy(source, sx, sz, col).start()

    forward(me, z, x)
    for i in range(N_DP - 1):
        k = pick(WAIT, i)
        to, sz, sx = ids(k)
        source = sz * NX + sx
        with jax.named_scope('w'):
            block_copy(to, k, source).wait_recv()
        forward(source, sz, sx)
        for j in range(NZ):
            if PLACED[j] == i:
                place(lax.rem(z - jnp.where(core == 0, PLANES[0][j], PLANES[1][j]) + NZ, NZ))
    with jax.named_scope('counted'):
        sent = pl.ds(0, N_DP - 1)
        pltpu.make_async_remote_copy(
            src_ref=send.at[sent], dst_ref=recv.at[sent], send_sem=send_sem, recv_sem=recv_sem.at[0],
            device_id={"dp": me}, device_id_type=MESH).wait_send()
        pltpu.make_async_remote_copy(
            src_ref=cnt_send.at[sent], dst_ref=cnt_recv.at[sent], send_sem=cs_sem, recv_sem=cr_sem,
            device_id={"dp": me}, device_id_type=MESH).wait()
    total = cnt_recv[0]
    for d in range(1, N_DP):
        total = total + cnt_recv[d]
    loads[...] = total

    away = lax.rem(z - col + NZ, NZ)
    late = jnp.int32(0)
    for dz in range(NZ):
        if DONE[1][dz] < DONE[0][dz]:
            late = jnp.where(away == dz, 1, late)

    def add(member, sx):
        block = share[member * NX + sx]
        for r in range(2):
            c = code_ref[r, member].astype(jnp.float32) * 0.25
            sums[r * NX + sx] = sums[r * NX + sx] + c * block

    for sx in range(NX):
        block = recv[col * NX + sx]
        for r in range(2):
            sums[r * NX + sx] = (code_ref[r, col].astype(jnp.float32) * 0.25) * block

    def shared(j, carry):
        other = 2 * lax.rem(j, 4) + lax.rem(late + lax.div(j, 4), 2)

        @pl.when(other != col)
        def _():
            for sx in range(NX):
                with jax.named_scope('s%d' % sx):
                    share_copy(other * NX + sx, sx, other, other).wait_recv()
                add(other, sx)
        return carry

    lax.fori_loop(0, N_PAR, shared, 0)
    for h in range(NX // 2):
        for r in range(2):
            one, two = sums[r * NX + 2 * h], sums[r * NX + 2 * h + 1]
            at = slice(h * PAIR, (h + 1) * PAIR)
            parity[at, (2 * r) * WIDTH:(2 * r + 1) * WIDTH] = jnp.concatenate([one[0:ROOM], two[0:ROOM]], axis=0)
            parity[at, (2 * r + 1) * WIDTH:(2 * r + 2) * WIDTH] = jnp.concatenate([one[ROOM:PAIR], two[ROOM:PAIR]], axis=0)

    with jax.named_scope('sent'):
        moved = pl.ds(0, (N_PAR - 1) * NX)
        pltpu.make_async_remote_copy(
            src_ref=recv.at[moved], dst_ref=share.at[moved], send_sem=ps_sem, recv_sem=pr_sem.at[0],
            device_id={"parity": col}, device_id_type=MESH).wait_send()


def put_out(nf, ns, par, cnt, nf_out, ns_out, par_out, cnt_out, sem):
    copies = []
    for src, dst, pieces in ((nf, nf_out, PIECES), (ns, ns_out, PIECES), (par, par_out, PIECES // 2)):
        rows = src.shape[0] // pieces
        for n in range(pieces):
            part = pl.ds(n * rows, rows)
            copies.append(pltpu.make_async_copy(src.at[part], dst.at[part], sem.at[len(copies)]))
    for c in copies:
        c.start()
    cnt_out[...] = cnt[0:1, 0:1]
    for c in copies:
        c.wait()


def body(first_moment, second_moment, new_owner, code_index):
    f32, i32 = jnp.float32, jnp.int32
    capacity = N_DP * ROOM
    vmem = pl.BlockSpec(memory_space=pltpu.VMEM)
    anywhere = pl.BlockSpec(memory_space=pl.ANY)
    hbm = pl.BlockSpec(memory_space=pltpu.HBM)
    dma = pltpu.SemaphoreType.DMA
    held = pl.pallas_call(
        exchange,
        out_shape=(jax.ShapeDtypeStruct((capacity, WIDTH), f32), jax.ShapeDtypeStruct((capacity, WIDTH), f32),
                   jax.ShapeDtypeStruct((capacity // N_PAR, 4 * WIDTH), f32), jax.ShapeDtypeStruct((1, 128), i32)),
        in_specs=[hbm, hbm, hbm, hbm],
        out_specs=(vmem, vmem, vmem, vmem),
        scratch_shapes=[
            pltpu.VMEM((1, BLK), i32), pltpu.SMEM((2, N_PAR), i32),
            pltpu.VMEM((BLK, WIDTH), f32), pltpu.VMEM((BLK, WIDTH), f32), pltpu.VMEM((6, BLK, WIDTH), jnp.bfloat16),
            pltpu.VMEM((N_DP, PAIR, WIDTH), f32), pltpu.VMEM((N_DP, PAIR, WIDTH), f32),
            pltpu.VMEM((N_PAR * NX, PAIR, WIDTH), f32), pltpu.VMEM((2 * NX, PAIR, WIDTH), f32),
            pltpu.VMEM((N_DP, 1, 128), i32), pltpu.VMEM((N_DP, 1, 128), i32),
            dma((4,)), dma, dma((N_DP,)), dma, dma, dma, dma((N_DP,)),
        ],
        compiler_params=pltpu.CompilerParams(collective_id=0, has_side_effects=True, vmem_limit_bytes=32 * 2**20),
    )(*(pltpu.with_memory_space_constraint(a, pltpu.HBM)
        for a in (first_moment, second_moment, new_owner.reshape(1, BLK), code_index)))
    return pl.pallas_call(
        put_out,
        out_shape=(jax.ShapeDtypeStruct((capacity, WIDTH), f32), jax.ShapeDtypeStruct((capacity, WIDTH), f32),
                   jax.ShapeDtypeStruct((capacity // N_PAR, 4 * WIDTH), f32), jax.ShapeDtypeStruct((1, 1), i32)),
        in_specs=[vmem, vmem, vmem, vmem],
        out_specs=(anywhere, anywhere, anywhere, vmem),
        scratch_shapes=[dma((2 * PIECES + PIECES // 2,))],
        compiler_params=pltpu.CompilerParams(vmem_limit_bytes=16 * 2**20),
    )(*held)


def solution(mesh):
    rows = P(("dp", "parity"), None)
    return jax.shard_map(body, mesh=mesh, in_specs=(rows, rows, rows, P()),
                         out_specs=(rows, rows, rows, P("dp", "parity")), check_vma=False)
```

```python
import functools

import jax
import jax.numpy as jnp
from jax import lax
from jax.experimental import pallas as pl
from jax.experimental.pallas import tpu as pltpu
from jax.sharding import PartitionSpec as P

MESH = pl.DeviceIdType.MESH
NZ, NX = 8, 4
N_DP = NZ * NX
N_PAR = 8
ROOM = 20
BLK = 512
WIDTH = 512
PAIR = 2 * ROOM
PIECES = 4
LANE = 32


def by_class(classes):
    steps = []
    for n, c in enumerate(classes):
        if n == 1:
            steps += [(0, dx) for dx in range(1, NX)]
        for dx in range(NX):
            steps += [(c, dx)] if 2 * c == NZ else [(c, dx), (NZ - c, dx)]
    return [dz * NX + dx for dz, dx in steps]


CLASSES = ((1, 2, 4, 3), (1, 4, 3, 2), (1, 3, 4, 2), (1, 4, 2, 3), (1, 3, 4, 2), (1, 4, 2, 3), (1, 3, 2, 4), (1, 3, 4, 2))
ISSUE = tuple(by_class(c) for c in CLASSES)
WAIT = ISSUE
DONE = tuple([max(w.index(k) for k in range(dz * NX, dz * NX + NX) if k) for dz in range(NZ)] for w in WAIT)
PLANES = tuple(sorted(range(NZ), key=done.__getitem__) for done in DONE)
PLACED = [max(done[planes[j]] for done, planes in zip(DONE, PLANES)) for j in range(NZ)]
MEMBERS = tuple(sorted(range(N_PAR), key=lambda p: DONE[p][dz]) for dz in range(NZ))


def exchange(first_hbm, second_hbm, owner_hbm, code_hbm,
             new_first, new_second, parity, loads,
             owner_ref, code_ref, x_first, x_second, parts, send, recv, share, sums, cnt_send, cnt_recv,
             in_sem, send_sem, recv_sem, cs_sem, cr_sem, ps_sem, pr_sem, ready):
    me = lax.axis_index("dp")
    col = lax.axis_index("parity")
    z = lax.div(me, NX)
    x = lax.rem(me, NX)

    loads_in = [
        pltpu.make_async_copy(first_hbm, x_first, in_sem.at[0]),
        pltpu.make_async_copy(second_hbm, x_second, in_sem.at[1]),
    ]
    small_in = [
        pltpu.make_async_copy(owner_hbm, owner_ref, in_sem.at[2]),
        pltpu.make_async_copy(code_hbm, code_ref, in_sem.at[3]),
    ]
    for c in small_in + loads_in:
        c.start()

    def at(dz, dx):
        return {"dp": lax.rem(z + dz + NZ, NZ) * NX + lax.rem(x + dx, NX)}

    near = [(dz, dx) for dz in (1, -1, 0) for dx in range(NX) if (dz, dx) != (0, 0)]
    barrier = pltpu.get_barrier_semaphore()
    for dz, dx in near:
        pl.semaphore_signal(barrier, inc=1, device_id=at(dz, dx), device_id_type=MESH)
    for k in range(1, N_PAR):
        pl.semaphore_signal(barrier, inc=1, device_id={"parity": lax.rem(col + k, N_PAR)}, device_id_type=MESH)

    def vouch(sem):
        for dz in (1, -1):
            pl.semaphore_signal(sem, inc=1, device_id=at(dz, 0), device_id_type=MESH)

    for c in small_in:
        c.wait()
    owner = owner_ref[...]
    onehot = (lax.broadcasted_iota(jnp.int32, (N_DP, BLK), 0) == owner).astype(jnp.float32)
    earlier = lax.broadcasted_iota(jnp.int32, (BLK, BLK), 0) < lax.broadcasted_iota(jnp.int32, (BLK, BLK), 1)
    before = jnp.dot(onehot.astype(jnp.bfloat16), earlier.astype(jnp.float32).astype(jnp.bfloat16),
                     preferred_element_type=jnp.float32)
    rank = jnp.sum(before * onehot, axis=0, keepdims=True)
    key = owner.astype(jnp.float32) * LANE + rank
    counts = jnp.sum(onehot, axis=1, keepdims=True).astype(jnp.int32)
    counts = jnp.broadcast_to(counts, (N_DP, 128))
    for d in range(N_DP):
        cnt_send[d] = counts[d:d + 1]

    for m, (c, src) in enumerate(zip(loads_in, (x_first, x_second))):
        c.wait()
        whole = src[...]
        high = whole.astype(jnp.bfloat16)
        rest = whole - high.astype(jnp.float32)
        mid = rest.astype(jnp.bfloat16)
        parts[3 * m] = high
        parts[3 * m + 1] = mid
        parts[3 * m + 2] = (rest - mid.astype(jnp.float32)).astype(jnp.bfloat16)

    rows = 24
    shape = (NX, rows, BLK)
    slot = (lax.broadcasted_iota(jnp.int32, shape, 0) * LANE + lax.broadcasted_iota(jnp.int32, shape, 1))
    slot = slot.reshape(NX * rows, BLK).astype(jnp.float32)

    def build(*planes):
        planes = [lax.rem(z + dz, NZ) for dz in planes]
        chosen = []
        for m in range(2):
            pick = jnp.concatenate([
                jnp.where(slot == key + (4 * m - p * (NX * LANE)).astype(jnp.float32), 1.0, 0.0) for p in planes
            ], axis=0).astype(jnp.bfloat16)
            out = jnp.dot(pick, parts[3 * m], preferred_element_type=jnp.float32)
            out = out + jnp.dot(pick, parts[3 * m + 1], preferred_element_type=jnp.float32)
            out = out + jnp.dot(pick, parts[3 * m + 2], preferred_element_type=jnp.float32)
            chosen.append(out.reshape(len(planes) * NX, rows, WIDTH))
        a, b = chosen
        for n, p in enumerate(planes):
            for o in range(NX):
                d, o = p * NX + o, n * NX + o
                send[d, 0:16] = a[o, 0:16]
                send[d, 16:24] = a[o, 16:24] + b[o, 0:8]
                send[d, 24:40] = b[o, 8:24]

    def ids(k):
        dz, dx = lax.div(k, NX), lax.rem(k, NX)
        to = lax.rem(z + dz, NZ) * NX + lax.rem(x + dx, NX)
        source_z = lax.rem(z - dz + NZ, NZ)
        source_x = lax.rem(x - dx + NX, NX)
        return to, source_z, source_x

    def pick(table, i, which=col):
        value = jnp.int32(table[0][i])
        for p in range(1, len(table)):
            if table[p][i] != table[0][i]:
                value = jnp.where(which == p, table[p][i], value)
        return value

    def block_copy(to, k, landing):
        return pltpu.make_async_remote_copy(
            src_ref=send.at[to], dst_ref=recv.at[landing], send_sem=send_sem, recv_sem=recv_sem.at[k],
            device_id={"dp": to}, device_id_type=MESH)

    def count_copy(to, landing):
        return pltpu.make_async_remote_copy(
            src_ref=cnt_send.at[to], dst_ref=cnt_recv.at[landing], send_sem=cs_sem, recv_sem=cr_sem,
            device_id={"dp": to}, device_id_type=MESH)

    def share_copy(source, source_x, target, from_col):
        return pltpu.make_async_remote_copy(
            src_ref=recv.at[source], dst_ref=share.at[from_col * NX + source_x],
            send_sem=ps_sem, recv_sem=pr_sem.at[from_col],
            device_id={"parity": target}, device_id_type=MESH)

    def issue(i):
        k = pick(ISSUE, i)
        to, _, _ = ids(k)
        block_copy(to, k, me).start()
        count_copy(to, me).start()

    with jax.named_scope('build1'):
        build(1, NZ - 1)
    with jax.named_scope('barrier'):
        pl.semaphore_wait(barrier, len(near) + N_PAR - 1)
    vouch(ready.at[0])
    for i in range(2 * NX):
        issue(i)
    for c in (2, 3):
        with jax.named_scope('build%d' % c):
            build(c, NZ - c)
        with jax.named_scope('ready%d' % c):
            pl.semaphore_wait(ready.at[c - 2], 2)
        vouch(ready.at[c - 1])
    with jax.named_scope('build4'):
        build(0, 4)
    with jax.named_scope('ready4'):
        pl.semaphore_wait(ready.at[2], 2)
    for i in range(2 * NX, N_DP - 1):
        issue(i)
    recv[me] = send[me]
    cnt_recv[me] = cnt_send[me]

    def place(sz):
        for h in range(NX // 2):
            one, two = sz * NX + 2 * h, sz * NX + 2 * h + 1
            at = pl.ds(pl.multiple_of((sz * (NX // 2) + h) * PAIR, 8), PAIR)
            new_first[at] = jnp.concatenate([recv[one, 0:ROOM], recv[two, 0:ROOM]], axis=0)
            new_second[at] = jnp.concatenate([recv[one, ROOM:PAIR], recv[two, ROOM:PAIR]], axis=0)

    def forward(source, sz, sx):
        @pl.when(sz != col)
        def _():
            share_copy(source, sx, sz, col).start()

    forward(me, z, x)
    for i in range(N_DP - 1):
        k = pick(WAIT, i)
        to, sz, sx = ids(k)
        source = sz * NX + sx
        with jax.named_scope('w'):
            block_copy(to, k, source).wait_recv()
        forward(source, sz, sx)
        for j in range(NZ):
            if PLACED[j] == i:
                place(lax.rem(z - pick(PLANES, j) + NZ, NZ))
    with jax.named_scope('counted'):
        sent = pl.ds(0, N_DP - 1)
        pltpu.make_async_remote_copy(
            src_ref=send.at[sent], dst_ref=recv.at[sent], send_sem=send_sem, recv_sem=recv_sem.at[0],
            device_id={"dp": me}, device_id_type=MESH).wait_send()
        pltpu.make_async_remote_copy(
            src_ref=cnt_send.at[sent], dst_ref=cnt_recv.at[sent], send_sem=cs_sem, recv_sem=cr_sem,
            device_id={"dp": me}, device_id_type=MESH).wait()
    total = cnt_recv[0]
    for d in range(1, N_DP):
        total = total + cnt_recv[d]
    loads[...] = total

    away = lax.rem(z - col + NZ, NZ)

    def add(member, sx):
        block = share[member * NX + sx]
        for r in range(2):
            c = code_ref[r, member].astype(jnp.float32) * 0.25
            sums[r * NX + sx] = sums[r * NX + sx] + c * block

    for sx in range(NX):
        block = recv[col * NX + sx]
        for r in range(2):
            sums[r * NX + sx] = (code_ref[r, col].astype(jnp.float32) * 0.25) * block

    for j in range(N_PAR):
        other = pick(MEMBERS, j, away)

        @pl.when(other != col)
        def _():
            four = pl.ds(other * NX, NX)
            with jax.named_scope('s'):
                pltpu.make_async_remote_copy(
                    src_ref=recv.at[four], dst_ref=share.at[four], send_sem=ps_sem, recv_sem=pr_sem.at[other],
                    device_id={"parity": other}, device_id_type=MESH).wait_recv()
            for sx in range(NX):
                add(other, sx)

    for h in range(NX // 2):
        for r in range(2):
            one, two = sums[r * NX + 2 * h], sums[r * NX + 2 * h + 1]
            at = slice(h * PAIR, (h + 1) * PAIR)
            parity[at, (2 * r) * WIDTH:(2 * r + 1) * WIDTH] = jnp.concatenate([one[0:ROOM], two[0:ROOM]], axis=0)
            parity[at, (2 * r + 1) * WIDTH:(2 * r + 2) * WIDTH] = jnp.concatenate([one[ROOM:PAIR], two[ROOM:PAIR]], axis=0)

    with jax.named_scope('sent'):
        moved = pl.ds(0, (N_PAR - 1) * NX)
        pltpu.make_async_remote_copy(
            src_ref=recv.at[moved], dst_ref=share.at[moved], send_sem=ps_sem, recv_sem=pr_sem.at[0],
            device_id={"parity": col}, device_id_type=MESH).wait_send()


def put_out(nf, ns, par, cnt, nf_out, ns_out, par_out, cnt_out, count, sem):
    count[...] = cnt[0:1, 0:1]
    copies = [pltpu.make_async_copy(count, cnt_out, sem.at[0])]
    for src, dst, pieces in ((nf, nf_out, PIECES), (ns, ns_out, PIECES), (par, par_out, PIECES // 2)):
        rows = src.shape[0] // pieces
        for n in range(pieces):
            part = pl.ds(n * rows, rows)
            copies.append(pltpu.make_async_copy(src.at[part], dst.at[part], sem.at[len(copies)]))
    for c in copies[1:] + copies[:1]:
        c.start()
    for c in copies:
        c.wait()


def body(first_moment, second_moment, new_owner, code_index):
    f32, i32 = jnp.float32, jnp.int32
    capacity = N_DP * ROOM
    vmem = pl.BlockSpec(memory_space=pltpu.VMEM)
    anywhere = pl.BlockSpec(memory_space=pl.ANY)
    hbm = pl.BlockSpec(memory_space=pltpu.HBM)
    dma = pltpu.SemaphoreType.DMA
    held = pl.pallas_call(
        exchange,
        out_shape=(jax.ShapeDtypeStruct((capacity, WIDTH), f32), jax.ShapeDtypeStruct((capacity, WIDTH), f32),
                   jax.ShapeDtypeStruct((capacity // N_PAR, 4 * WIDTH), f32), jax.ShapeDtypeStruct((1, 128), i32)),
        in_specs=[hbm, hbm, hbm, hbm],
        out_specs=(vmem, vmem, vmem, vmem),
        scratch_shapes=[
            pltpu.VMEM((1, BLK), i32), pltpu.SMEM((2, N_PAR), i32),
            pltpu.VMEM((BLK, WIDTH), f32), pltpu.VMEM((BLK, WIDTH), f32), pltpu.VMEM((6, BLK, WIDTH), jnp.bfloat16),
            pltpu.VMEM((N_DP, PAIR, WIDTH), f32), pltpu.VMEM((N_DP, PAIR, WIDTH), f32),
            pltpu.VMEM((N_PAR * NX, PAIR, WIDTH), f32), pltpu.VMEM((2 * NX, PAIR, WIDTH), f32),
            pltpu.VMEM((N_DP, 1, 128), i32), pltpu.VMEM((N_DP, 1, 128), i32),
            dma((4,)), dma, dma((N_DP,)), dma, dma, dma, dma((N_PAR,)), pltpu.SemaphoreType.REGULAR((3,)),
        ],
        compiler_params=pltpu.CompilerParams(collective_id=0, has_side_effects=True, vmem_limit_bytes=32 * 2**20),
    )(*(pltpu.with_memory_space_constraint(a, pltpu.HBM)
        for a in (first_moment, second_moment, new_owner.reshape(1, BLK), code_index)))
    return pl.pallas_call(
        put_out,
        out_shape=(jax.ShapeDtypeStruct((capacity, WIDTH), f32), jax.ShapeDtypeStruct((capacity, WIDTH), f32),
                   jax.ShapeDtypeStruct((capacity // N_PAR, 4 * WIDTH), f32), jax.ShapeDtypeStruct((1, 1), i32)),
        in_specs=[vmem, vmem, vmem, vmem],
        out_specs=(anywhere, anywhere, anywhere, anywhere),
        scratch_shapes=[pltpu.VMEM((1, 1), i32), dma((1 + 2 * PIECES + PIECES // 2,))],
        compiler_params=pltpu.CompilerParams(vmem_limit_bytes=16 * 2**20),
    )(*held)


def solution(mesh):
    rows = P(("dp", "parity"), None)
    return jax.shard_map(body, mesh=mesh, in_specs=(rows, rows, rows, P()),
                         out_specs=(rows, rows, rows, P("dp", "parity")), check_vma=False)
```

```python
import functools

import jax
import jax.numpy as jnp
from jax import lax
from jax.experimental import pallas as pl
from jax.experimental.pallas import tpu as pltpu
from jax.sharding import PartitionSpec as P

MESH = pl.DeviceIdType.MESH
NZ, NX = 8, 4
N_DP = NZ * NX
N_PAR = 8
ROOM = 20
BLK = 512
WIDTH = 512
PAIR = 2 * ROOM
PIECES = 4
LANE = 32


ISSUE = (
    (4, 28, 5, 29, 6, 30, 7, 31, 1, 2, 3, 9, 25, 17, 13, 21, 11, 27, 19, 15, 23, 10, 26, 18, 14, 22, 8, 24, 16, 12, 20),
    (4, 28, 5, 29, 6, 30, 7, 31, 1, 2, 3, 12, 20, 16, 8, 24, 13, 21, 17, 9, 25, 14, 22, 18, 10, 26, 15, 23, 19, 11, 27),
    (4, 28, 5, 29, 6, 30, 7, 31, 1, 2, 3, 17, 13, 21, 9, 25, 19, 15, 23, 11, 27, 18, 14, 22, 10, 26, 16, 12, 20, 8, 24),
    (4, 28, 5, 29, 6, 30, 7, 31, 1, 2, 3, 8, 24, 12, 20, 16, 9, 25, 13, 21, 17, 10, 26, 14, 22, 18, 11, 27, 15, 23, 19),
    (4, 28, 5, 29, 6, 30, 7, 31, 1, 2, 3, 13, 21, 9, 25, 17, 15, 23, 11, 27, 19, 14, 22, 10, 26, 18, 12, 20, 8, 24, 16),
    (4, 28, 5, 29, 6, 30, 7, 31, 1, 2, 3, 16, 8, 24, 12, 20, 17, 9, 25, 15, 23, 13, 21, 18, 10, 26, 19, 14, 22, 11, 27),
    (4, 28, 5, 29, 6, 30, 7, 31, 1, 2, 3, 9, 25, 17, 13, 21, 11, 27, 19, 15, 23, 10, 26, 18, 14, 22, 8, 24, 16, 12, 20),
    (4, 28, 5, 29, 6, 30, 7, 31, 1, 2, 3, 12, 20, 16, 8, 24, 13, 21, 17, 9, 25, 14, 22, 18, 10, 26, 15, 23, 19, 11, 27),
)
WAIT = ISSUE
DONE = tuple([max(w.index(k) for k in range(dz * NX, dz * NX + NX) if k) for dz in range(NZ)] for w in WAIT)
PLANES = tuple(sorted(range(NZ), key=done.__getitem__) for done in DONE)
PLACED = [max(done[planes[j]] for done, planes in zip(DONE, PLANES)) for j in range(NZ)]
MEMBERS = tuple(sorted(range(N_PAR), key=lambda p: DONE[p][dz]) for dz in range(NZ))


def exchange(first_hbm, second_hbm, owner_hbm, code_hbm,
             new_first, new_second, sums, loads,
             owner_ref, code_ref, x_first, x_second, earlier, parts, send, recv, share, cnt_send, cnt_recv,
             in_sem, send_sem, recv_sem, cs_sem, cr_sem, ps_sem, pr_sem, ready):
    me = lax.axis_index("dp")
    col = lax.axis_index("parity")
    z = lax.div(me, NX)
    x = lax.rem(me, NX)

    loads_in = [
        pltpu.make_async_copy(first_hbm, x_first, in_sem.at[0]),
        pltpu.make_async_copy(second_hbm, x_second, in_sem.at[1]),
    ]
    small_in = [
        pltpu.make_async_copy(owner_hbm, owner_ref, in_sem.at[2]),
        pltpu.make_async_copy(code_hbm, code_ref, in_sem.at[3]),
    ]
    for c in small_in + loads_in:
        c.start()

    def at(dz, dx):
        return {"dp": lax.rem(z + dz + NZ, NZ) * NX + lax.rem(x + dx, NX)}

    near = [(dz, dx) for dz in (1, -1, 0) for dx in range(NX) if (dz, dx) != (0, 0)]
    barrier = pltpu.get_barrier_semaphore()
    for dz, dx in near:
        pl.semaphore_signal(barrier, inc=1, device_id=at(dz, dx), device_id_type=MESH)
    for k in range(1, N_PAR):
        pl.semaphore_signal(barrier, inc=1, device_id={"parity": lax.rem(col + k, N_PAR)}, device_id_type=MESH)

    def vouch(sem):
        for dz in (1, -1):
            pl.semaphore_signal(sem, inc=1, device_id=at(dz, 0), device_id_type=MESH)

    earlier[...] = (lax.broadcasted_iota(jnp.int32, (BLK, BLK), 0)
                    < lax.broadcasted_iota(jnp.int32, (BLK, BLK), 1)).astype(jnp.float32).astype(jnp.bfloat16)
    for c in small_in:
        c.wait()
    owner = owner_ref[...]
    onehot = (lax.broadcasted_iota(jnp.int32, (N_DP, BLK), 0) == owner).astype(jnp.float32)
    before = jnp.dot(onehot.astype(jnp.bfloat16), earlier[...], preferred_element_type=jnp.float32)
    rank = jnp.sum(before * onehot, axis=0, keepdims=True)
    key = owner.astype(jnp.float32) * LANE + rank

    rows = 24
    shape = (NX, rows, BLK)
    slot = (lax.broadcasted_iota(jnp.int32, shape, 0) * LANE + lax.broadcasted_iota(jnp.int32, shape, 1))
    slot = slot.reshape(NX * rows, BLK).astype(jnp.float32)

    def choose(m, planes):
        chosen = jnp.concatenate([
            jnp.where(slot == key + (4 * m - p * (NX * LANE)).astype(jnp.float32), 1.0, 0.0) for p in planes
        ], axis=0).astype(jnp.bfloat16)
        out = jnp.dot(chosen, parts[3 * m], preferred_element_type=jnp.float32)
        out = out + jnp.dot(chosen, parts[3 * m + 1], preferred_element_type=jnp.float32)
        out = out + jnp.dot(chosen, parts[3 * m + 2], preferred_element_type=jnp.float32)
        return out.reshape(len(planes) * NX, rows, WIDTH)

    def fill(planes, a, b):
        for n, p in enumerate(planes):
            for o in range(NX):
                d, o = p * NX + o, n * NX + o
                send[d, 0:16] = a[o, 0:16]
                send[d, 16:24] = a[o, 16:24] + b[o, 0:8]
                send[d, 24:40] = b[o, 8:24]

    def planes_at(*distances):
        return [lax.rem(z + dz, NZ) for dz in distances]

    def build(*distances):
        planes = planes_at(*distances)
        fill(planes, choose(0, planes), choose(1, planes))

    beside, built = planes_at(1, NZ - 1), []
    for m, (c, src) in enumerate(zip(loads_in, (x_first, x_second))):
        c.wait()
        whole = src[...]
        high = whole.astype(jnp.bfloat16)
        rest = whole - high.astype(jnp.float32)
        mid = rest.astype(jnp.bfloat16)
        parts[3 * m] = high
        parts[3 * m + 1] = mid
        parts[3 * m + 2] = (rest - mid.astype(jnp.float32)).astype(jnp.bfloat16)
        built.append(choose(m, beside))
    fill(beside, *built)

    def ids(k):
        dz, dx = lax.div(k, NX), lax.rem(k, NX)
        to = lax.rem(z + dz, NZ) * NX + lax.rem(x + dx, NX)
        source_z = lax.rem(z - dz + NZ, NZ)
        source_x = lax.rem(x - dx + NX, NX)
        return to, source_z, source_x

    def pick(table, i, which=col):
        value = jnp.int32(table[0][i])
        for p in range(1, len(table)):
            if table[p][i] != table[0][i]:
                value = jnp.where(which == p, table[p][i], value)
        return value

    def block_copy(to, k, landing):
        return pltpu.make_async_remote_copy(
            src_ref=send.at[to], dst_ref=recv.at[landing], send_sem=send_sem, recv_sem=recv_sem.at[k],
            device_id={"dp": to}, device_id_type=MESH)

    def count_copy(to, landing):
        return pltpu.make_async_remote_copy(
            src_ref=cnt_send.at[to], dst_ref=cnt_recv.at[landing], send_sem=cs_sem, recv_sem=cr_sem,
            device_id={"dp": to}, device_id_type=MESH)

    def share_copy(source, source_x, target, from_col):
        return pltpu.make_async_remote_copy(
            src_ref=recv.at[source], dst_ref=share.at[from_col * NX + source_x],
            send_sem=ps_sem, recv_sem=pr_sem.at[from_col],
            device_id={"parity": target}, device_id_type=MESH)

    def issue(i):
        k = pick(ISSUE, i)
        to, _, _ = ids(k)
        block_copy(to, k, me).start()
        count_copy(to, me).start()

    counts = jnp.sum(onehot, axis=1, keepdims=True).astype(jnp.int32)
    counts = jnp.broadcast_to(counts, (N_DP, 128))
    for d in range(N_DP):
        cnt_send[d] = counts[d:d + 1]
    with jax.named_scope('barrier'):
        pl.semaphore_wait(barrier, len(near) + N_PAR - 1)
    vouch(ready.at[0])
    for i in range(2 * NX):
        issue(i)
    for c in (2, 3):
        with jax.named_scope('build%d' % c):
            build(c, NZ - c)
        with jax.named_scope('ready%d' % c):
            pl.semaphore_wait(ready.at[c - 2], 2)
        vouch(ready.at[c - 1])
    with jax.named_scope('build4'):
        build(0, 4)
    with jax.named_scope('ready4'):
        pl.semaphore_wait(ready.at[2], 2)
    for i in range(2 * NX, N_DP - 1):
        issue(i)
    recv[me] = send[me]
    cnt_recv[me] = cnt_send[me]

    def place(sz):
        for h in range(NX // 2):
            one, two = sz * NX + 2 * h, sz * NX + 2 * h + 1
            at = pl.ds(pl.multiple_of((sz * (NX // 2) + h) * PAIR, 8), PAIR)
            new_first[at] = jnp.concatenate([recv[one, 0:ROOM], recv[two, 0:ROOM]], axis=0)
            new_second[at] = jnp.concatenate([recv[one, ROOM:PAIR], recv[two, ROOM:PAIR]], axis=0)

    def forward(source, sz, sx):
        @pl.when(sz != col)
        def _():
            share_copy(source, sx, sz, col).start()

    forward(me, z, x)
    for i in range(N_DP - 1):
        k = pick(WAIT, i)
        to, sz, sx = ids(k)
        source = sz * NX + sx
        with jax.named_scope('w'):
            block_copy(to, k, source).wait_recv()
        forward(source, sz, sx)
        for j in range(NZ):
            if PLACED[j] == i:
                place(lax.rem(z - pick(PLANES, j) + NZ, NZ))
    with jax.named_scope('counted'):
        sent = pl.ds(0, N_DP - 1)
        pltpu.make_async_remote_copy(
            src_ref=send.at[sent], dst_ref=recv.at[sent], send_sem=send_sem, recv_sem=recv_sem.at[0],
            device_id={"dp": me}, device_id_type=MESH).wait_send()
        pltpu.make_async_remote_copy(
            src_ref=cnt_send.at[sent], dst_ref=cnt_recv.at[sent], send_sem=cs_sem, recv_sem=cr_sem,
            device_id={"dp": me}, device_id_type=MESH).wait()
    total = cnt_recv[0]
    for d in range(1, N_DP):
        total = total + cnt_recv[d]
    loads[...] = total

    away = lax.rem(z - col + NZ, NZ)

    def add(member, sx):
        block = share[member * NX + sx]
        for r in range(2):
            c = code_ref[r, member].astype(jnp.float32) * 0.25
            sums[r * NX + sx] = sums[r * NX + sx] + c * block

    for sx in range(NX):
        block = recv[col * NX + sx]
        for r in range(2):
            sums[r * NX + sx] = (code_ref[r, col].astype(jnp.float32) * 0.25) * block

    for j in range(N_PAR):
        other = pick(MEMBERS, j, away)

        @pl.when(other != col)
        def _():
            four = pl.ds(other * NX, NX)
            with jax.named_scope('s'):
                pltpu.make_async_remote_copy(
                    src_ref=recv.at[four], dst_ref=share.at[four], send_sem=ps_sem, recv_sem=pr_sem.at[other],
                    device_id={"parity": other}, device_id_type=MESH).wait_recv()
            for sx in range(NX):
                add(other, sx)

    with jax.named_scope('sent'):
        moved = pl.ds(0, (N_PAR - 1) * NX)
        pltpu.make_async_remote_copy(
            src_ref=recv.at[moved], dst_ref=share.at[moved], send_sem=ps_sem, recv_sem=pr_sem.at[0],
            device_id={"parity": col}, device_id_type=MESH).wait_send()


def put_out(nf, ns, sums, cnt, nf_out, ns_out, par_out, cnt_out, count, parity, sem):
    copies = []
    for src, dst in ((nf, nf_out), (ns, ns_out)):
        rows = src.shape[0] // PIECES
        for n in range(PIECES):
            part = pl.ds(n * rows, rows)
            copies.append(pltpu.make_async_copy(src.at[part], dst.at[part], sem.at[len(copies)]))
            copies[-1].start()
    count[...] = cnt[0:1, 0:1]
    copies.append(pltpu.make_async_copy(count, cnt_out, sem.at[len(copies)]))
    copies[-1].start()
    for h in range(NX // 2):
        for r in range(2):
            one, two = sums[r * NX + 2 * h], sums[r * NX + 2 * h + 1]
            at = slice(h * PAIR, (h + 1) * PAIR)
            parity[at, (2 * r) * WIDTH:(2 * r + 1) * WIDTH] = jnp.concatenate([one[0:ROOM], two[0:ROOM]], axis=0)
            parity[at, (2 * r + 1) * WIDTH:(2 * r + 2) * WIDTH] = jnp.concatenate([one[ROOM:PAIR], two[ROOM:PAIR]], axis=0)
        part = pl.ds(h * PAIR, PAIR)
        copies.append(pltpu.make_async_copy(parity.at[part], par_out.at[part], sem.at[len(copies)]))
        copies[-1].start()
    for c in copies:
        c.wait()


def body(first_moment, second_moment, new_owner, code_index):
    f32, i32 = jnp.float32, jnp.int32
    capacity = N_DP * ROOM
    vmem = pl.BlockSpec(memory_space=pltpu.VMEM)
    anywhere = pl.BlockSpec(memory_space=pl.ANY)
    hbm = pl.BlockSpec(memory_space=pltpu.HBM)
    dma = pltpu.SemaphoreType.DMA
    held = pl.pallas_call(
        exchange,
        out_shape=(jax.ShapeDtypeStruct((capacity, WIDTH), f32), jax.ShapeDtypeStruct((capacity, WIDTH), f32),
                   jax.ShapeDtypeStruct((2 * NX, PAIR, WIDTH), f32), jax.ShapeDtypeStruct((1, 128), i32)),
        in_specs=[hbm, hbm, hbm, hbm],
        out_specs=(vmem, vmem, vmem, vmem),
        scratch_shapes=[
            pltpu.VMEM((1, BLK), i32), pltpu.SMEM((2, N_PAR), i32),
            pltpu.VMEM((BLK, WIDTH), f32), pltpu.VMEM((BLK, WIDTH), f32), pltpu.VMEM((BLK, BLK), jnp.bfloat16),
            pltpu.VMEM((6, BLK, WIDTH), jnp.bfloat16),
            pltpu.VMEM((N_DP, PAIR, WIDTH), f32), pltpu.VMEM((N_DP, PAIR, WIDTH), f32),
            pltpu.VMEM((N_PAR * NX, PAIR, WIDTH), f32),
            pltpu.VMEM((N_DP, 1, 128), i32), pltpu.VMEM((N_DP, 1, 128), i32),
            dma((4,)), dma, dma((N_DP,)), dma, dma, dma, dma((N_PAR,)), pltpu.SemaphoreType.REGULAR((3,)),
        ],
        compiler_params=pltpu.CompilerParams(collective_id=0, has_side_effects=True, vmem_limit_bytes=32 * 2**20),
    )(*(pltpu.with_memory_space_constraint(a, pltpu.HBM)
        for a in (first_moment, second_moment, new_owner.reshape(1, BLK), code_index)))
    return pl.pallas_call(
        put_out,
        out_shape=(jax.ShapeDtypeStruct((capacity, WIDTH), f32), jax.ShapeDtypeStruct((capacity, WIDTH), f32),
                   jax.ShapeDtypeStruct((capacity // N_PAR, 4 * WIDTH), f32), jax.ShapeDtypeStruct((1, 1), i32)),
        in_specs=[vmem, vmem, vmem, vmem],
        out_specs=(anywhere, anywhere, anywhere, anywhere),
        scratch_shapes=[pltpu.VMEM((1, 1), i32), pltpu.VMEM((capacity // N_PAR, 4 * WIDTH), f32),
                        dma((2 * PIECES + 1 + NX // 2,))],
        compiler_params=pltpu.CompilerParams(vmem_limit_bytes=16 * 2**20),
    )(*held)


def solution(mesh):
    rows = P(("dp", "parity"), None)
    return jax.shard_map(body, mesh=mesh, in_specs=(rows, rows, rows, P()),
                         out_specs=(rows, rows, rows, P("dp", "parity")), check_vma=False)
```

```python
import functools

import jax
import jax.numpy as jnp
from jax import lax
from jax.experimental import pallas as pl
from jax.experimental.pallas import tpu as pltpu
from jax.sharding import PartitionSpec as P

MESH = pl.DeviceIdType.MESH
NZ, NX = 8, 4
N_DP = NZ * NX
N_PAR = 8
ROOM = 20
BLK = 512
WIDTH = 512
PAIR = 2 * ROOM
PIECES = 4
LANE = 32


ISSUE = (
    (4, 28, 5, 29, 6, 30, 7, 31, 1, 2, 3, 9, 25, 17, 13, 21, 11, 27, 19, 15, 23, 10, 26, 18, 14, 22, 8, 24, 16, 12, 20),
    (4, 28, 5, 29, 6, 30, 7, 31, 1, 2, 3, 12, 20, 16, 8, 24, 13, 21, 17, 9, 25, 14, 22, 18, 10, 26, 15, 23, 19, 11, 27),
    (4, 28, 5, 29, 6, 30, 7, 31, 1, 2, 3, 17, 13, 21, 9, 25, 19, 15, 23, 11, 27, 18, 14, 22, 10, 26, 16, 12, 20, 8, 24),
    (4, 28, 5, 29, 6, 30, 7, 31, 1, 2, 3, 16, 17, 18, 19, 8, 24, 9, 25, 10, 26, 11, 27, 12, 20, 13, 21, 14, 22, 15, 23),
    (4, 28, 5, 29, 6, 30, 7, 31, 1, 2, 3, 13, 21, 9, 25, 17, 15, 23, 11, 27, 19, 14, 22, 10, 26, 18, 12, 20, 8, 24, 16),
    (4, 28, 5, 29, 6, 30, 7, 31, 1, 2, 3, 16, 8, 24, 12, 20, 17, 9, 25, 15, 23, 13, 21, 18, 10, 26, 19, 14, 22, 11, 27),
    (4, 28, 5, 29, 6, 30, 7, 31, 1, 2, 3, 9, 25, 17, 13, 21, 11, 27, 19, 15, 23, 10, 26, 18, 14, 22, 8, 24, 16, 12, 20),
    (4, 28, 5, 29, 6, 30, 7, 31, 1, 2, 3, 12, 20, 16, 8, 24, 13, 21, 17, 9, 25, 14, 22, 18, 10, 26, 15, 23, 19, 11, 27),
)
WAIT = ISSUE
DONE = tuple([max(w.index(k) for k in range(dz * NX, dz * NX + NX) if k) for dz in range(NZ)] for w in WAIT)
PLANES = tuple(sorted(range(NZ), key=done.__getitem__) for done in DONE)
PLACED = [max(done[planes[j]] for done, planes in zip(DONE, PLANES)) for j in range(NZ)]
MEMBERS = tuple(sorted(range(N_PAR), key=lambda p: DONE[p][dz]) for dz in range(NZ))


def exchange(first_hbm, second_hbm, owner_hbm, code_hbm,
             new_first, new_second, sums, loads,
             owner_ref, code_ref, x_first, x_second, earlier, parts, send, recv, share, cnt_send, cnt_recv,
             in_sem, send_sem, recv_sem, cs_sem, cr_sem, ps_sem, pr_sem, ready):
    me = lax.axis_index("dp")
    col = lax.axis_index("parity")
    z = lax.div(me, NX)
    x = lax.rem(me, NX)

    loads_in = [
        pltpu.make_async_copy(first_hbm, x_first, in_sem.at[0]),
        pltpu.make_async_copy(second_hbm, x_second, in_sem.at[1]),
    ]
    small_in = [
        pltpu.make_async_copy(owner_hbm, owner_ref, in_sem.at[2]),
        pltpu.make_async_copy(code_hbm, code_ref, in_sem.at[3]),
    ]
    for c in small_in + loads_in:
        c.start()

    def at(dz, dx):
        return {"dp": lax.rem(z + dz + NZ, NZ) * NX + lax.rem(x + dx, NX)}

    near = [(dz, dx) for dz in (1, -1, 0) for dx in range(NX) if (dz, dx) != (0, 0)]
    barrier = pltpu.get_barrier_semaphore()
    for dz, dx in near:
        pl.semaphore_signal(barrier, inc=1, device_id=at(dz, dx), device_id_type=MESH)
    for k in range(1, N_PAR):
        pl.semaphore_signal(barrier, inc=1, device_id={"parity": lax.rem(col + k, N_PAR)}, device_id_type=MESH)

    def vouch(sem):
        for dz in (1, -1):
            pl.semaphore_signal(sem, inc=1, device_id=at(dz, 0), device_id_type=MESH)

    earlier[...] = (lax.broadcasted_iota(jnp.int32, (BLK, BLK), 0)
                    < lax.broadcasted_iota(jnp.int32, (BLK, BLK), 1)).astype(jnp.float32).astype(jnp.bfloat16)
    for c in small_in:
        c.wait()
    owner = owner_ref[...]
    onehot = (lax.broadcasted_iota(jnp.int32, (N_DP, BLK), 0) == owner).astype(jnp.float32)
    before = jnp.dot(onehot.astype(jnp.bfloat16), earlier[...], preferred_element_type=jnp.float32)
    rank = jnp.sum(before * onehot, axis=0, keepdims=True)
    key = owner.astype(jnp.float32) * LANE + rank

    rows = 24
    shape = (NX, rows, BLK)
    slot = (lax.broadcasted_iota(jnp.int32, shape, 0) * LANE + lax.broadcasted_iota(jnp.int32, shape, 1))
    slot = slot.reshape(NX * rows, BLK).astype(jnp.float32)

    def choose(m, planes):
        chosen = jnp.concatenate([
            jnp.where(slot == key + (4 * m - p * (NX * LANE)).astype(jnp.float32), 1.0, 0.0) for p in planes
        ], axis=0).astype(jnp.bfloat16)
        out = jnp.dot(chosen, parts[3 * m], preferred_element_type=jnp.float32)
        out = out + jnp.dot(chosen, parts[3 * m + 1], preferred_element_type=jnp.float32)
        out = out + jnp.dot(chosen, parts[3 * m + 2], preferred_element_type=jnp.float32)
        return out.reshape(len(planes) * NX, rows, WIDTH)

    def fill(planes, a, b):
        for n, p in enumerate(planes):
            for o in range(NX):
                d, o = p * NX + o, n * NX + o
                send[d, 0:16] = a[o, 0:16]
                send[d, 16:24] = a[o, 16:24] + b[o, 0:8]
                send[d, 24:40] = b[o, 8:24]

    def planes_at(*distances):
        return [lax.rem(z + dz, NZ) for dz in distances]

    def build(*distances):
        planes = planes_at(*distances)
        fill(planes, choose(0, planes), choose(1, planes))

    beside, built = planes_at(1, NZ - 1), []
    for m, (c, src) in enumerate(zip(loads_in, (x_first, x_second))):
        c.wait()
        whole = src[...]
        high = whole.astype(jnp.bfloat16)
        rest = whole - high.astype(jnp.float32)
        mid = rest.astype(jnp.bfloat16)
        parts[3 * m] = high
        parts[3 * m + 1] = mid
        parts[3 * m + 2] = (rest - mid.astype(jnp.float32)).astype(jnp.bfloat16)
        built.append(choose(m, beside))
    fill(beside, *built)

    def ids(k):
        dz, dx = lax.div(k, NX), lax.rem(k, NX)
        to = lax.rem(z + dz, NZ) * NX + lax.rem(x + dx, NX)
        source_z = lax.rem(z - dz + NZ, NZ)
        source_x = lax.rem(x - dx + NX, NX)
        return to, source_z, source_x

    def pick(table, i, which=col):
        value = jnp.int32(table[0][i])
        for p in range(1, len(table)):
            if table[p][i] != table[0][i]:
                value = jnp.where(which == p, table[p][i], value)
        return value

    def block_copy(to, k, landing):
        return pltpu.make_async_remote_copy(
            src_ref=send.at[to], dst_ref=recv.at[landing], send_sem=send_sem, recv_sem=recv_sem.at[k],
            device_id={"dp": to}, device_id_type=MESH)

    def count_copy(to, landing):
        return pltpu.make_async_remote_copy(
            src_ref=cnt_send.at[to], dst_ref=cnt_recv.at[landing], send_sem=cs_sem, recv_sem=cr_sem,
            device_id={"dp": to}, device_id_type=MESH)

    def share_copy(source, source_x, target, from_col):
        return pltpu.make_async_remote_copy(
            src_ref=recv.at[source], dst_ref=share.at[from_col * NX + source_x],
            send_sem=ps_sem, recv_sem=pr_sem.at[from_col],
            device_id={"parity": target}, device_id_type=MESH)

    def issue(i):
        k = pick(ISSUE, i)
        to, _, _ = ids(k)
        block_copy(to, k, me).start()
        count_copy(to, me).start()

    counts = jnp.sum(onehot, axis=1, keepdims=True).astype(jnp.int32)
    counts = jnp.broadcast_to(counts, (N_DP, 128))
    for d in range(N_DP):
        cnt_send[d] = counts[d:d + 1]
    with jax.named_scope('barrier'):
        pl.semaphore_wait(barrier, len(near) + N_PAR - 1)
    vouch(ready.at[0])
    for i in range(2 * NX):
        issue(i)
    for c in (2, 3):
        with jax.named_scope('build%d' % c):
            build(c, NZ - c)
        with jax.named_scope('ready%d' % c):
            pl.semaphore_wait(ready.at[c - 2], 2)
        vouch(ready.at[c - 1])
    with jax.named_scope('build4'):
        build(0, 4)
    with jax.named_scope('ready4'):
        pl.semaphore_wait(ready.at[2], 2)
    for i in range(2 * NX, N_DP - 1):
        issue(i)
    recv[me] = send[me]
    cnt_recv[me] = cnt_send[me]

    def place(sz):
        for h in range(NX // 2):
            one, two = sz * NX + 2 * h, sz * NX + 2 * h + 1
            at = pl.ds(pl.multiple_of((sz * (NX // 2) + h) * PAIR, 8), PAIR)
            new_first[at] = jnp.concatenate([recv[one, 0:ROOM], recv[two, 0:ROOM]], axis=0)
            new_second[at] = jnp.concatenate([recv[one, ROOM:PAIR], recv[two, ROOM:PAIR]], axis=0)

    def forward(source, sz, sx):
        @pl.when(sz != col)
        def _():
            share_copy(source, sx, sz, col).start()

    forward(me, z, x)
    for i in range(N_DP - 1):
        k = pick(WAIT, i)
        to, sz, sx = ids(k)
        source = sz * NX + sx
        with jax.named_scope('w'):
            block_copy(to, k, source).wait_recv()
        forward(source, sz, sx)
        for j in range(NZ):
            if PLACED[j] == i:
                place(lax.rem(z - pick(PLANES, j) + NZ, NZ))
    with jax.named_scope('counted'):
        sent = pl.ds(0, N_DP - 1)
        pltpu.make_async_remote_copy(
            src_ref=send.at[sent], dst_ref=recv.at[sent], send_sem=send_sem, recv_sem=recv_sem.at[0],
            device_id={"dp": me}, device_id_type=MESH).wait_send()
        pltpu.make_async_remote_copy(
            src_ref=cnt_send.at[sent], dst_ref=cnt_recv.at[sent], send_sem=cs_sem, recv_sem=cr_sem,
            device_id={"dp": me}, device_id_type=MESH).wait()
    total = cnt_recv[0]
    for d in range(1, N_DP):
        total = total + cnt_recv[d]
    loads[...] = total

    away = lax.rem(z - col + NZ, NZ)

    def add(member, sx):
        block = share[member * NX + sx]
        for r in range(2):
            c = code_ref[r, member].astype(jnp.float32) * 0.25
            sums[r * NX + sx] = sums[r * NX + sx] + c * block

    for sx in range(NX):
        block = recv[col * NX + sx]
        for r in range(2):
            sums[r * NX + sx] = (code_ref[r, col].astype(jnp.float32) * 0.25) * block

    for j in range(N_PAR):
        other = pick(MEMBERS, j, away)

        @pl.when(other != col)
        def _():
            four = pl.ds(other * NX, NX)
            with jax.named_scope('s'):
                pltpu.make_async_remote_copy(
                    src_ref=recv.at[four], dst_ref=share.at[four], send_sem=ps_sem, recv_sem=pr_sem.at[other],
                    device_id={"parity": other}, device_id_type=MESH).wait_recv()
            for sx in range(NX):
                add(other, sx)

    with jax.named_scope('sent'):
        moved = pl.ds(0, (N_PAR - 1) * NX)
        pltpu.make_async_remote_copy(
            src_ref=recv.at[moved], dst_ref=share.at[moved], send_sem=ps_sem, recv_sem=pr_sem.at[0],
            device_id={"parity": col}, device_id_type=MESH).wait_send()


def put_out(nf, ns, sums, cnt, nf_out, ns_out, par_out, cnt_out, count, parity, sem):
    copies = []
    for src, dst in ((nf, nf_out), (ns, ns_out)):
        rows = src.shape[0] // PIECES
        for n in range(PIECES):
            part = pl.ds(n * rows, rows)
            copies.append(pltpu.make_async_copy(src.at[part], dst.at[part], sem.at[len(copies)]))
            copies[-1].start()
    count[...] = cnt[0:1, 0:1]
    copies.append(pltpu.make_async_copy(count, cnt_out, sem.at[len(copies)]))
    copies[-1].start()
    for h in range(NX // 2):
        for r in range(2):
            one, two = sums[r * NX + 2 * h], sums[r * NX + 2 * h + 1]
            at = slice(h * PAIR, (h + 1) * PAIR)
            parity[at, (2 * r) * WIDTH:(2 * r + 1) * WIDTH] = jnp.concatenate([one[0:ROOM], two[0:ROOM]], axis=0)
            parity[at, (2 * r + 1) * WIDTH:(2 * r + 2) * WIDTH] = jnp.concatenate([one[ROOM:PAIR], two[ROOM:PAIR]], axis=0)
        part = pl.ds(h * PAIR, PAIR)
        copies.append(pltpu.make_async_copy(parity.at[part], par_out.at[part], sem.at[len(copies)]))
        copies[-1].start()
    for c in copies:
        c.wait()


def body(first_moment, second_moment, new_owner, code_index):
    f32, i32 = jnp.float32, jnp.int32
    capacity = N_DP * ROOM
    vmem = pl.BlockSpec(memory_space=pltpu.VMEM)
    anywhere = pl.BlockSpec(memory_space=pl.ANY)
    hbm = pl.BlockSpec(memory_space=pltpu.HBM)
    dma = pltpu.SemaphoreType.DMA
    held = pl.pallas_call(
        exchange,
        out_shape=(jax.ShapeDtypeStruct((capacity, WIDTH), f32), jax.ShapeDtypeStruct((capacity, WIDTH), f32),
                   jax.ShapeDtypeStruct((2 * NX, PAIR, WIDTH), f32), jax.ShapeDtypeStruct((1, 128), i32)),
        in_specs=[hbm, hbm, hbm, hbm],
        out_specs=(vmem, vmem, vmem, vmem),
        scratch_shapes=[
            pltpu.VMEM((1, BLK), i32), pltpu.SMEM((2, N_PAR), i32),
            pltpu.VMEM((BLK, WIDTH), f32), pltpu.VMEM((BLK, WIDTH), f32), pltpu.VMEM((BLK, BLK), jnp.bfloat16),
            pltpu.VMEM((6, BLK, WIDTH), jnp.bfloat16),
            pltpu.VMEM((N_DP, PAIR, WIDTH), f32), pltpu.VMEM((N_DP, PAIR, WIDTH), f32),
            pltpu.VMEM((N_PAR * NX, PAIR, WIDTH), f32),
            pltpu.VMEM((N_DP, 1, 128), i32), pltpu.VMEM((N_DP, 1, 128), i32),
            dma((4,)), dma, dma((N_DP,)), dma, dma, dma, dma((N_PAR,)), pltpu.SemaphoreType.REGULAR((3,)),
        ],
        compiler_params=pltpu.CompilerParams(collective_id=0, has_side_effects=True, vmem_limit_bytes=32 * 2**20),
    )(*(pltpu.with_memory_space_constraint(a, pltpu.HBM)
        for a in (first_moment, second_moment, new_owner.reshape(1, BLK), code_index)))
    return pl.pallas_call(
        put_out,
        out_shape=(jax.ShapeDtypeStruct((capacity, WIDTH), f32), jax.ShapeDtypeStruct((capacity, WIDTH), f32),
                   jax.ShapeDtypeStruct((capacity // N_PAR, 4 * WIDTH), f32), jax.ShapeDtypeStruct((1, 1), i32)),
        in_specs=[vmem, vmem, vmem, vmem],
        out_specs=(anywhere, anywhere, anywhere, anywhere),
        scratch_shapes=[pltpu.VMEM((1, 1), i32), pltpu.VMEM((capacity // N_PAR, 4 * WIDTH), f32),
                        dma((2 * PIECES + 1 + NX // 2,))],
        compiler_params=pltpu.CompilerParams(vmem_limit_bytes=16 * 2**20),
    )(*held)


def solution(mesh):
    rows = P(("dp", "parity"), None)
    return jax.shard_map(body, mesh=mesh, in_specs=(rows, rows, rows, P()),
                         out_specs=(rows, rows, rows, P("dp", "parity")), check_vma=False)
```

```python
import functools

import jax
import jax.numpy as jnp
from jax import lax
from jax.experimental import pallas as pl
from jax.experimental.pallas import tpu as pltpu
from jax.sharding import PartitionSpec as P

MESH = pl.DeviceIdType.MESH
NZ, NX = 8, 4
N_DP = NZ * NX
N_PAR = 8
ROOM = 20
BLK = 512
WIDTH = 512
PAIR = 2 * ROOM
PIECES = 1
LANE = 32


ISSUE = (
    (4, 28, 5, 29, 6, 30, 7, 31, 1, 2, 3, 9, 25, 17, 13, 21, 11, 27, 19, 15, 23, 10, 26, 18, 14, 22, 8, 24, 16, 12, 20),
    (4, 28, 5, 29, 6, 30, 7, 31, 1, 2, 3, 12, 20, 16, 8, 24, 13, 21, 17, 9, 25, 14, 22, 18, 10, 26, 15, 23, 19, 11, 27),
    (4, 28, 5, 29, 6, 30, 7, 31, 1, 2, 3, 17, 13, 21, 9, 25, 19, 15, 23, 11, 27, 18, 14, 22, 10, 26, 16, 12, 20, 8, 24),
    (4, 28, 5, 29, 6, 30, 7, 31, 1, 2, 3, 16, 17, 18, 19, 8, 24, 9, 25, 10, 26, 11, 27, 12, 20, 13, 21, 14, 22, 15, 23),
    (4, 28, 5, 29, 6, 30, 7, 31, 1, 2, 3, 13, 21, 9, 25, 17, 15, 23, 11, 27, 19, 14, 22, 10, 26, 18, 12, 20, 8, 24, 16),
    (4, 28, 5, 29, 6, 30, 7, 31, 1, 2, 3, 16, 8, 24, 12, 20, 17, 9, 25, 15, 23, 13, 21, 18, 10, 26, 19, 14, 22, 11, 27),
    (4, 28, 5, 29, 6, 30, 7, 31, 1, 2, 3, 9, 25, 17, 13, 21, 11, 27, 19, 15, 23, 10, 26, 18, 14, 22, 8, 24, 16, 12, 20),
    (4, 28, 5, 29, 6, 30, 7, 31, 1, 2, 3, 12, 20, 16, 8, 24, 13, 21, 17, 9, 25, 14, 22, 18, 10, 26, 15, 23, 19, 11, 27),
)
WAIT = ISSUE
DONE = tuple([max(w.index(k) for k in range(dz * NX, dz * NX + NX) if k) for dz in range(NZ)] for w in WAIT)
PLANES = tuple(sorted(range(NZ), key=done.__getitem__) for done in DONE)
PLACED = [max(done[planes[j]] for done, planes in zip(DONE, PLANES)) for j in range(NZ)]
MEMBERS = tuple(sorted(range(N_PAR), key=lambda p: DONE[p][dz]) for dz in range(NZ))


def exchange(first_hbm, second_hbm, owner_hbm, code_hbm,
             new_first, new_second, sums, loads,
             owner_ref, code_ref, x_first, x_second, earlier, parts, send, recv, share, cnt_send, cnt_recv,
             in_sem, send_sem, recv_sem, cs_sem, cr_sem, ps_sem, pr_sem, ready):
    me = lax.axis_index("dp")
    col = lax.axis_index("parity")
    z = lax.div(me, NX)
    x = lax.rem(me, NX)

    loads_in = [
        pltpu.make_async_copy(first_hbm, x_first, in_sem.at[0]),
        pltpu.make_async_copy(second_hbm, x_second, in_sem.at[1]),
    ]
    small_in = [
        pltpu.make_async_copy(owner_hbm, owner_ref, in_sem.at[2]),
        pltpu.make_async_copy(code_hbm, code_ref, in_sem.at[3]),
    ]
    for c in small_in + loads_in:
        c.start()

    def at(dz, dx):
        return {"dp": lax.rem(z + dz + NZ, NZ) * NX + lax.rem(x + dx, NX)}

    near = [(dz, dx) for dz in (1, -1, 0) for dx in range(NX) if (dz, dx) != (0, 0)]
    barrier = pltpu.get_barrier_semaphore()
    for dz, dx in near:
        pl.semaphore_signal(barrier, inc=1, device_id=at(dz, dx), device_id_type=MESH)
    for k in range(1, N_PAR):
        pl.semaphore_signal(barrier, inc=1, device_id={"parity": lax.rem(col + k, N_PAR)}, device_id_type=MESH)

    def vouch(sem):
        for dz in (1, -1):
            pl.semaphore_signal(sem, inc=1, device_id=at(dz, 0), device_id_type=MESH)

    earlier[...] = (lax.broadcasted_iota(jnp.int32, (BLK, BLK), 0)
                    < lax.broadcasted_iota(jnp.int32, (BLK, BLK), 1)).astype(jnp.float32).astype(jnp.bfloat16)
    for c in small_in:
        c.wait()
    owner = owner_ref[...]
    onehot = (lax.broadcasted_iota(jnp.int32, (N_DP, BLK), 0) == owner).astype(jnp.float32)
    before = jnp.dot(onehot.astype(jnp.bfloat16), earlier[...], preferred_element_type=jnp.float32)
    rank = jnp.sum(before * onehot, axis=0, keepdims=True)
    key = owner.astype(jnp.float32) * LANE + rank

    rows = 24
    shape = (NX, rows, BLK)
    slot = (lax.broadcasted_iota(jnp.int32, shape, 0) * LANE + lax.broadcasted_iota(jnp.int32, shape, 1))
    slot = slot.reshape(NX * rows, BLK).astype(jnp.float32)

    def choose(m, planes):
        chosen = jnp.concatenate([
            jnp.where(slot == key + (4 * m - p * (NX * LANE)).astype(jnp.float32), 1.0, 0.0) for p in planes
        ], axis=0).astype(jnp.bfloat16)
        out = jnp.dot(chosen, parts[3 * m], preferred_element_type=jnp.float32)
        out = out + jnp.dot(chosen, parts[3 * m + 1], preferred_element_type=jnp.float32)
        out = out + jnp.dot(chosen, parts[3 * m + 2], preferred_element_type=jnp.float32)
        return out.reshape(len(planes) * NX, rows, WIDTH)

    def fill(planes, a, b):
        for n, p in enumerate(planes):
            for o in range(NX):
                d, o = p * NX + o, n * NX + o
                send[d, 0:16] = a[o, 0:16]
                send[d, 16:24] = a[o, 16:24] + b[o, 0:8]
                send[d, 24:40] = b[o, 8:24]

    def planes_at(*distances):
        return [lax.rem(z + dz, NZ) for dz in distances]

    def build(*distances):
        planes = planes_at(*distances)
        fill(planes, choose(0, planes), choose(1, planes))

    beside, built = planes_at(1, NZ - 1), []
    for m, (c, src) in enumerate(zip(loads_in, (x_first, x_second))):
        c.wait()
        whole = src[...]
        high = whole.astype(jnp.bfloat16)
        rest = whole - high.astype(jnp.float32)
        mid = rest.astype(jnp.bfloat16)
        parts[3 * m] = high
        parts[3 * m + 1] = mid
        parts[3 * m + 2] = (rest - mid.astype(jnp.float32)).astype(jnp.bfloat16)
        built.append(choose(m, beside))
    fill(beside, *built)

    def ids(k):
        dz, dx = lax.div(k, NX), lax.rem(k, NX)
        to = lax.rem(z + dz, NZ) * NX + lax.rem(x + dx, NX)
        source_z = lax.rem(z - dz + NZ, NZ)
        source_x = lax.rem(x - dx + NX, NX)
        return to, source_z, source_x

    def pick(table, i, which=col):
        value = jnp.int32(table[0][i])
        for p in range(1, len(table)):
            if table[p][i] != table[0][i]:
                value = jnp.where(which == p, table[p][i], value)
        return value

    def block_copy(to, k, landing):
        return pltpu.make_async_remote_copy(
            src_ref=send.at[to], dst_ref=recv.at[landing], send_sem=send_sem, recv_sem=recv_sem.at[k],
            device_id={"dp": to}, device_id_type=MESH)

    def count_copy(to, landing):
        return pltpu.make_async_remote_copy(
            src_ref=cnt_send.at[to], dst_ref=cnt_recv.at[landing], send_sem=cs_sem, recv_sem=cr_sem,
            device_id={"dp": to}, device_id_type=MESH)

    def share_copy(source, source_x, target, from_col):
        return pltpu.make_async_remote_copy(
            src_ref=recv.at[source], dst_ref=share.at[from_col * NX + source_x],
            send_sem=ps_sem, recv_sem=pr_sem.at[from_col],
            device_id={"parity": target}, device_id_type=MESH)

    def issue(i):
        k = pick(ISSUE, i)
        to, _, _ = ids(k)
        block_copy(to, k, me).start()

    with jax.named_scope('barrier'):
        pl.semaphore_wait(barrier, len(near) + N_PAR - 1)
    vouch(ready.at[0])
    for i in range(2 * NX):
        issue(i)
    counts = jnp.sum(onehot, axis=1, keepdims=True).astype(jnp.int32)
    counts = jnp.broadcast_to(counts, (N_DP, 128))
    for d in range(N_DP):
        cnt_send[d] = counts[d:d + 1]
    for c in (2, 3):
        with jax.named_scope('build%d' % c):
            build(c, NZ - c)
        with jax.named_scope('ready%d' % c):
            pl.semaphore_wait(ready.at[c - 2], 2)
        vouch(ready.at[c - 1])
    with jax.named_scope('build4'):
        build(0, 4)
    with jax.named_scope('ready4'):
        pl.semaphore_wait(ready.at[2], 2)
    for i in range(2 * NX, N_DP - 1):
        issue(i)
    for i in range(N_DP - 1):
        to, _, _ = ids(pick(ISSUE, i))
        count_copy(to, me).start()
    recv[me] = send[me]
    cnt_recv[me] = cnt_send[me]

    def place(sz):
        for h in range(NX // 2):
            one, two = sz * NX + 2 * h, sz * NX + 2 * h + 1
            at = pl.ds(pl.multiple_of((sz * (NX // 2) + h) * PAIR, 8), PAIR)
            new_first[at] = jnp.concatenate([recv[one, 0:ROOM], recv[two, 0:ROOM]], axis=0)
            new_second[at] = jnp.concatenate([recv[one, ROOM:PAIR], recv[two, ROOM:PAIR]], axis=0)

    def forward(source, sz, sx):
        @pl.when(sz != col)
        def _():
            share_copy(source, sx, sz, col).start()

    forward(me, z, x)
    for i in range(N_DP - 1):
        k = pick(WAIT, i)
        to, sz, sx = ids(k)
        source = sz * NX + sx
        with jax.named_scope('w'):
            block_copy(to, k, source).wait_recv()
        forward(source, sz, sx)
        for j in range(NZ):
            if PLACED[j] == i:
                place(lax.rem(z - pick(PLANES, j) + NZ, NZ))
    with jax.named_scope('counted'):
        sent = pl.ds(0, N_DP - 1)
        pltpu.make_async_remote_copy(
            src_ref=send.at[sent], dst_ref=recv.at[sent], send_sem=send_sem, recv_sem=recv_sem.at[0],
            device_id={"dp": me}, device_id_type=MESH).wait_send()
        pltpu.make_async_remote_copy(
            src_ref=cnt_send.at[sent], dst_ref=cnt_recv.at[sent], send_sem=cs_sem, recv_sem=cr_sem,
            device_id={"dp": me}, device_id_type=MESH).wait()
    total = cnt_recv[0]
    for d in range(1, N_DP):
        total = total + cnt_recv[d]
    loads[...] = total

    away = lax.rem(z - col + NZ, NZ)

    def add(member, sx):
        block = share[member * NX + sx]
        for r in range(2):
            c = code_ref[r, member].astype(jnp.float32) * 0.25
            sums[r * NX + sx] = sums[r * NX + sx] + c * block

    for sx in range(NX):
        block = recv[col * NX + sx]
        for r in range(2):
            sums[r * NX + sx] = (code_ref[r, col].astype(jnp.float32) * 0.25) * block

    for j in range(N_PAR):
        other = pick(MEMBERS, j, away)

        @pl.when(other != col)
        def _():
            four = pl.ds(other * NX, NX)
            with jax.named_scope('s'):
                pltpu.make_async_remote_copy(
                    src_ref=recv.at[four], dst_ref=share.at[four], send_sem=ps_sem, recv_sem=pr_sem.at[other],
                    device_id={"parity": other}, device_id_type=MESH).wait_recv()
            for sx in range(NX):
                add(other, sx)

    with jax.named_scope('sent'):
        moved = pl.ds(0, (N_PAR - 1) * NX)
        pltpu.make_async_remote_copy(
            src_ref=recv.at[moved], dst_ref=share.at[moved], send_sem=ps_sem, recv_sem=pr_sem.at[0],
            device_id={"parity": col}, device_id_type=MESH).wait_send()


def put_out(nf, ns, sums, cnt, nf_out, ns_out, par_out, cnt_out, count, parity, sem):
    copies = []
    for src, dst in ((nf, nf_out), (ns, ns_out)):
        rows = src.shape[0] // PIECES
        for n in range(PIECES):
            part = pl.ds(n * rows, rows)
            copies.append(pltpu.make_async_copy(src.at[part], dst.at[part], sem.at[len(copies)]))
            copies[-1].start()
    count[...] = cnt[0:1, 0:1]
    copies.append(pltpu.make_async_copy(count, cnt_out, sem.at[len(copies)]))
    copies[-1].start()
    for h in range(NX // 2):
        for r in range(2):
            one, two = sums[r * NX + 2 * h], sums[r * NX + 2 * h + 1]
            at = slice(h * PAIR, (h + 1) * PAIR)
            parity[at, (2 * r) * WIDTH:(2 * r + 1) * WIDTH] = jnp.concatenate([one[0:ROOM], two[0:ROOM]], axis=0)
            parity[at, (2 * r + 1) * WIDTH:(2 * r + 2) * WIDTH] = jnp.concatenate([one[ROOM:PAIR], two[ROOM:PAIR]], axis=0)
        part = pl.ds(h * PAIR, PAIR)
        copies.append(pltpu.make_async_copy(parity.at[part], par_out.at[part], sem.at[len(copies)]))
        copies[-1].start()
    for c in copies:
        c.wait()


def body(first_moment, second_moment, new_owner, code_index):
    f32, i32 = jnp.float32, jnp.int32
    capacity = N_DP * ROOM
    vmem = pl.BlockSpec(memory_space=pltpu.VMEM)
    anywhere = pl.BlockSpec(memory_space=pl.ANY)
    hbm = pl.BlockSpec(memory_space=pltpu.HBM)
    dma = pltpu.SemaphoreType.DMA
    held = pl.pallas_call(
        exchange,
        out_shape=(jax.ShapeDtypeStruct((capacity, WIDTH), f32), jax.ShapeDtypeStruct((capacity, WIDTH), f32),
                   jax.ShapeDtypeStruct((2 * NX, PAIR, WIDTH), f32), jax.ShapeDtypeStruct((1, 128), i32)),
        in_specs=[hbm, hbm, hbm, hbm],
        out_specs=(vmem, vmem, vmem, vmem),
        scratch_shapes=[
            pltpu.VMEM((1, BLK), i32), pltpu.SMEM((2, N_PAR), i32),
            pltpu.VMEM((BLK, WIDTH), f32), pltpu.VMEM((BLK, WIDTH), f32), pltpu.VMEM((BLK, BLK), jnp.bfloat16),
            pltpu.VMEM((6, BLK, WIDTH), jnp.bfloat16),
            pltpu.VMEM((N_DP, PAIR, WIDTH), f32), pltpu.VMEM((N_DP, PAIR, WIDTH), f32),
            pltpu.VMEM((N_PAR * NX, PAIR, WIDTH), f32),
            pltpu.VMEM((N_DP, 1, 128), i32), pltpu.VMEM((N_DP, 1, 128), i32),
            dma((4,)), dma, dma((N_DP,)), dma, dma, dma, dma((N_PAR,)), pltpu.SemaphoreType.REGULAR((3,)),
        ],
        compiler_params=pltpu.CompilerParams(collective_id=0, has_side_effects=True, vmem_limit_bytes=32 * 2**20),
    )(*(pltpu.with_memory_space_constraint(a, pltpu.HBM)
        for a in (first_moment, second_moment, new_owner.reshape(1, BLK), code_index)))
    return pl.pallas_call(
        put_out,
        out_shape=(jax.ShapeDtypeStruct((capacity, WIDTH), f32), jax.ShapeDtypeStruct((capacity, WIDTH), f32),
                   jax.ShapeDtypeStruct((capacity // N_PAR, 4 * WIDTH), f32), jax.ShapeDtypeStruct((1, 1), i32)),
        in_specs=[vmem, vmem, vmem, vmem],
        out_specs=(anywhere, anywhere, anywhere, anywhere),
        scratch_shapes=[pltpu.VMEM((1, 1), i32), pltpu.VMEM((capacity // N_PAR, 4 * WIDTH), f32),
                        dma((2 * PIECES + 1 + NX // 2,))],
        compiler_params=pltpu.CompilerParams(vmem_limit_bytes=16 * 2**20),
    )(*held)


def solution(mesh):
    rows = P(("dp", "parity"), None)
    return jax.shard_map(body, mesh=mesh, in_specs=(rows, rows, rows, P()),
                         out_specs=(rows, rows, rows, P("dp", "parity")), check_vma=False)
```

```python
import functools

import jax
import jax.numpy as jnp
from jax import lax
from jax.experimental import pallas as pl
from jax.experimental.pallas import tpu as pltpu
from jax.sharding import PartitionSpec as P

MESH = pl.DeviceIdType.MESH
NZ, NX = 8, 4
N_DP = NZ * NX
N_PAR = 8
ROOM = 20
BLK = 512
WIDTH = 512
PAIR = 2 * ROOM
PIECES = 1
LANE = 32


ISSUE = (
    (4, 28, 5, 29, 6, 30, 7, 31, 1, 2, 3, 9, 25, 17, 13, 21, 11, 27, 19, 15, 23, 10, 26, 18, 14, 22, 8, 24, 16, 12, 20),
    (4, 28, 5, 29, 6, 30, 7, 31, 1, 2, 3, 12, 20, 16, 8, 24, 13, 21, 17, 9, 25, 14, 22, 18, 10, 26, 15, 23, 19, 11, 27),
    (4, 28, 5, 29, 6, 30, 7, 31, 1, 2, 3, 17, 13, 21, 9, 25, 19, 15, 23, 11, 27, 18, 14, 22, 10, 26, 16, 12, 20, 8, 24),
    (4, 28, 5, 29, 6, 30, 7, 31, 1, 2, 3, 16, 17, 18, 19, 8, 24, 9, 25, 10, 26, 11, 27, 12, 20, 13, 21, 14, 22, 15, 23),
    (4, 28, 5, 29, 6, 30, 7, 31, 1, 2, 3, 13, 21, 9, 25, 17, 15, 23, 11, 27, 19, 14, 22, 10, 26, 18, 12, 20, 8, 24, 16),
    (4, 28, 5, 29, 6, 30, 7, 31, 1, 2, 3, 16, 8, 24, 12, 20, 17, 9, 25, 15, 23, 13, 21, 18, 10, 26, 19, 14, 22, 11, 27),
    (4, 28, 5, 29, 6, 30, 7, 31, 1, 2, 3, 9, 25, 17, 13, 21, 11, 27, 19, 15, 23, 10, 26, 18, 14, 22, 8, 24, 16, 12, 20),
    (4, 28, 5, 29, 6, 30, 7, 31, 1, 2, 3, 12, 20, 16, 8, 24, 13, 21, 17, 9, 25, 14, 22, 18, 10, 26, 15, 23, 19, 11, 27),
)
WAIT = ISSUE
DONE = tuple([max(w.index(k) for k in range(dz * NX, dz * NX + NX) if k) for dz in range(NZ)] for w in WAIT)
PLANES = tuple(sorted(range(NZ), key=done.__getitem__) for done in DONE)
PLACED = [max(done[planes[j]] for done, planes in zip(DONE, PLANES)) for j in range(NZ)]
MEMBERS = tuple(sorted(range(N_PAR), key=lambda p: DONE[p][dz]) for dz in range(NZ))


def exchange(first_hbm, second_hbm, owner_hbm, code_hbm,
             new_first, new_second, sums, loads,
             owner_ref, code_ref, x_first, x_second, earlier, parts, send, recv, share, cnt_send, cnt_recv,
             in_sem, send_sem, recv_sem, cs_sem, cr_sem, ps_sem, pr_sem, ready):
    me = lax.axis_index("dp")
    col = lax.axis_index("parity")
    z = lax.div(me, NX)
    x = lax.rem(me, NX)

    loads_in = [
        pltpu.make_async_copy(first_hbm, x_first, in_sem.at[0]),
        pltpu.make_async_copy(second_hbm, x_second, in_sem.at[1]),
    ]
    small_in = [
        pltpu.make_async_copy(owner_hbm, owner_ref, in_sem.at[2]),
        pltpu.make_async_copy(code_hbm, code_ref, in_sem.at[3]),
    ]
    for c in small_in + loads_in:
        c.start()

    def at(dz, dx):
        return {"dp": lax.rem(z + dz + NZ, NZ) * NX + lax.rem(x + dx, NX)}

    near = [(dz, dx) for dz in (1, -1, 0) for dx in range(NX) if (dz, dx) != (0, 0)]
    barrier = pltpu.get_barrier_semaphore()
    for dz, dx in near:
        pl.semaphore_signal(barrier, inc=1, device_id=at(dz, dx), device_id_type=MESH)
    for k in range(1, N_PAR):
        pl.semaphore_signal(barrier, inc=1, device_id={"parity": lax.rem(col + k, N_PAR)}, device_id_type=MESH)

    def vouch(sem):
        for dz in (1, -1):
            pl.semaphore_signal(sem, inc=1, device_id=at(dz, 0), device_id_type=MESH)

    earlier[...] = (lax.broadcasted_iota(jnp.int32, (BLK, BLK), 0)
                    < lax.broadcasted_iota(jnp.int32, (BLK, BLK), 1)).astype(jnp.float32).astype(jnp.bfloat16)
    for c in small_in:
        c.wait()
    owner = owner_ref[...]
    onehot = (lax.broadcasted_iota(jnp.int32, (N_DP, BLK), 0) == owner).astype(jnp.float32)
    before = jnp.dot(onehot.astype(jnp.bfloat16), earlier[...], preferred_element_type=jnp.float32)
    rank = jnp.sum(before * onehot, axis=0, keepdims=True)
    key = owner.astype(jnp.float32) * LANE + rank

    rows = 24
    shape = (NX, rows, BLK)
    slot = (lax.broadcasted_iota(jnp.int32, shape, 0) * LANE + lax.broadcasted_iota(jnp.int32, shape, 1))
    slot = slot.reshape(NX * rows, BLK).astype(jnp.float32)

    def choose(m, planes):
        chosen = jnp.concatenate([
            jnp.where(slot == key + (4 * m - p * (NX * LANE)).astype(jnp.float32), 1.0, 0.0) for p in planes
        ], axis=0).astype(jnp.bfloat16)
        out = jnp.dot(chosen, parts[3 * m], preferred_element_type=jnp.float32)
        out = out + jnp.dot(chosen, parts[3 * m + 1], preferred_element_type=jnp.float32)
        out = out + jnp.dot(chosen, parts[3 * m + 2], preferred_element_type=jnp.float32)
        return out.reshape(len(planes) * NX, rows, WIDTH)

    def fill(planes, a, b):
        for n, p in enumerate(planes):
            for o in range(NX):
                d, o = p * NX + o, n * NX + o
                send[d, 0:16] = a[o, 0:16]
                send[d, 16:24] = a[o, 16:24] + b[o, 0:8]
                send[d, 24:40] = b[o, 8:24]

    def planes_at(*distances):
        return [lax.rem(z + dz, NZ) for dz in distances]

    def build(*distances):
        planes = planes_at(*distances)
        fill(planes, choose(0, planes), choose(1, planes))

    beside, built = planes_at(1, NZ - 1), []
    for m, (c, src) in enumerate(zip(loads_in, (x_first, x_second))):
        c.wait()
        whole = src[...]
        high = whole.astype(jnp.bfloat16)
        rest = whole - high.astype(jnp.float32)
        mid = rest.astype(jnp.bfloat16)
        parts[3 * m] = high
        parts[3 * m + 1] = mid
        parts[3 * m + 2] = (rest - mid.astype(jnp.float32)).astype(jnp.bfloat16)
        built.append(choose(m, beside))
    fill(beside, *built)

    def ids(k):
        dz, dx = lax.div(k, NX), lax.rem(k, NX)
        to = lax.rem(z + dz, NZ) * NX + lax.rem(x + dx, NX)
        source_z = lax.rem(z - dz + NZ, NZ)
        source_x = lax.rem(x - dx + NX, NX)
        return to, source_z, source_x

    def pick(table, i, which=col):
        value = jnp.int32(table[0][i])
        for p in range(1, len(table)):
            if table[p][i] != table[0][i]:
                value = jnp.where(which == p, table[p][i], value)
        return value

    def block_copy(to, k, landing):
        return pltpu.make_async_remote_copy(
            src_ref=send.at[to], dst_ref=recv.at[landing], send_sem=send_sem, recv_sem=recv_sem.at[k],
            device_id={"dp": to}, device_id_type=MESH)

    def count_copy(to, landing):
        return pltpu.make_async_remote_copy(
            src_ref=cnt_send.at[to], dst_ref=cnt_recv.at[landing], send_sem=cs_sem, recv_sem=cr_sem,
            device_id={"dp": to}, device_id_type=MESH)

    def share_copy(source, source_x, target, from_col):
        return pltpu.make_async_remote_copy(
            src_ref=recv.at[source], dst_ref=share.at[from_col * NX + source_x],
            send_sem=ps_sem, recv_sem=pr_sem.at[from_col],
            device_id={"parity": target}, device_id_type=MESH)

    def issue(i):
        k = pick(ISSUE, i)
        to, _, _ = ids(k)
        block_copy(to, k, me).start()

    with jax.named_scope('barrier'):
        pl.semaphore_wait(barrier, len(near) + N_PAR - 1)
    vouch(ready.at[0])
    for i in range(2 * NX):
        issue(i)
    counts = jnp.sum(onehot, axis=1, keepdims=True).astype(jnp.int32)
    counts = jnp.broadcast_to(counts, (N_DP, 128))
    for d in range(N_DP):
        cnt_send[d] = counts[d:d + 1]
    for c in (2, 3):
        with jax.named_scope('ready%d' % c):
            pl.semaphore_wait(ready.at[c - 2], 2)
        vouch(ready.at[c - 1])
        with jax.named_scope('build%d' % c):
            build(c, NZ - c)
    with jax.named_scope('build4'):
        build(0, 4)
    with jax.named_scope('ready4'):
        pl.semaphore_wait(ready.at[2], 2)
    for i in range(2 * NX, N_DP - 1):
        issue(i)
    for i in range(N_DP - 1):
        to, _, _ = ids(pick(ISSUE, i))
        count_copy(to, me).start()
    recv[me] = send[me]
    cnt_recv[me] = cnt_send[me]

    def place(sz):
        for h in range(NX // 2):
            one, two = sz * NX + 2 * h, sz * NX + 2 * h + 1
            at = pl.ds(pl.multiple_of((sz * (NX // 2) + h) * PAIR, 8), PAIR)
            new_first[at] = jnp.concatenate([recv[one, 0:ROOM], recv[two, 0:ROOM]], axis=0)
            new_second[at] = jnp.concatenate([recv[one, ROOM:PAIR], recv[two, ROOM:PAIR]], axis=0)

    def forward(source, sz, sx):
        @pl.when(sz != col)
        def _():
            share_copy(source, sx, sz, col).start()

    forward(me, z, x)
    for i in range(N_DP - 1):
        k = pick(WAIT, i)
        to, sz, sx = ids(k)
        source = sz * NX + sx
        with jax.named_scope('w'):
            block_copy(to, k, source).wait_recv()
        forward(source, sz, sx)
        for j in range(NZ):
            if PLACED[j] == i:
                place(lax.rem(z - pick(PLANES, j) + NZ, NZ))
    with jax.named_scope('counted'):
        sent = pl.ds(0, N_DP - 1)
        pltpu.make_async_remote_copy(
            src_ref=send.at[sent], dst_ref=recv.at[sent], send_sem=send_sem, recv_sem=recv_sem.at[0],
            device_id={"dp": me}, device_id_type=MESH).wait_send()
        pltpu.make_async_remote_copy(
            src_ref=cnt_send.at[sent], dst_ref=cnt_recv.at[sent], send_sem=cs_sem, recv_sem=cr_sem,
            device_id={"dp": me}, device_id_type=MESH).wait()
    total = cnt_recv[0]
    for d in range(1, N_DP):
        total = total + cnt_recv[d]
    loads[...] = total

    away = lax.rem(z - col + NZ, NZ)

    def add(member, sx):
        block = share[member * NX + sx]
        for r in range(2):
            c = code_ref[r, member].astype(jnp.float32) * 0.25
            sums[r * NX + sx] = sums[r * NX + sx] + c * block

    for sx in range(NX):
        block = recv[col * NX + sx]
        for r in range(2):
            sums[r * NX + sx] = (code_ref[r, col].astype(jnp.float32) * 0.25) * block

    for j in range(N_PAR):
        other = pick(MEMBERS, j, away)

        @pl.when(other != col)
        def _():
            four = pl.ds(other * NX, NX)
            with jax.named_scope('s'):
                pltpu.make_async_remote_copy(
                    src_ref=recv.at[four], dst_ref=share.at[four], send_sem=ps_sem, recv_sem=pr_sem.at[other],
                    device_id={"parity": other}, device_id_type=MESH).wait_recv()
            for sx in range(NX):
                add(other, sx)

    with jax.named_scope('sent'):
        moved = pl.ds(0, (N_PAR - 1) * NX)
        pltpu.make_async_remote_copy(
            src_ref=recv.at[moved], dst_ref=share.at[moved], send_sem=ps_sem, recv_sem=pr_sem.at[0],
            device_id={"parity": col}, device_id_type=MESH).wait_send()


def put_out(nf, ns, sums, cnt, nf_out, ns_out, par_out, cnt_out, count, parity, sem):
    copies = []
    for src, dst in ((nf, nf_out), (ns, ns_out)):
        rows = src.shape[0] // PIECES
        for n in range(PIECES):
            part = pl.ds(n * rows, rows)
            copies.append(pltpu.make_async_copy(src.at[part], dst.at[part], sem.at[len(copies)]))
            copies[-1].start()
    count[...] = cnt[0:1, 0:1]
    copies.append(pltpu.make_async_copy(count, cnt_out, sem.at[len(copies)]))
    copies[-1].start()
    for h in range(NX // 2):
        for r in range(2):
            one, two = sums[r * NX + 2 * h], sums[r * NX + 2 * h + 1]
            at = slice(h * PAIR, (h + 1) * PAIR)
            parity[at, (2 * r) * WIDTH:(2 * r + 1) * WIDTH] = jnp.concatenate([one[0:ROOM], two[0:ROOM]], axis=0)
            parity[at, (2 * r + 1) * WIDTH:(2 * r + 2) * WIDTH] = jnp.concatenate([one[ROOM:PAIR], two[ROOM:PAIR]], axis=0)
        part = pl.ds(h * PAIR, PAIR)
        copies.append(pltpu.make_async_copy(parity.at[part], par_out.at[part], sem.at[len(copies)]))
        copies[-1].start()
    for c in copies:
        c.wait()


def body(first_moment, second_moment, new_owner, code_index):
    f32, i32 = jnp.float32, jnp.int32
    capacity = N_DP * ROOM
    vmem = pl.BlockSpec(memory_space=pltpu.VMEM)
    anywhere = pl.BlockSpec(memory_space=pl.ANY)
    hbm = pl.BlockSpec(memory_space=pltpu.HBM)
    dma = pltpu.SemaphoreType.DMA
    held = pl.pallas_call(
        exchange,
        out_shape=(jax.ShapeDtypeStruct((capacity, WIDTH), f32), jax.ShapeDtypeStruct((capacity, WIDTH), f32),
                   jax.ShapeDtypeStruct((2 * NX, PAIR, WIDTH), f32), jax.ShapeDtypeStruct((1, 128), i32)),
        in_specs=[hbm, hbm, hbm, hbm],
        out_specs=(vmem, vmem, vmem, vmem),
        scratch_shapes=[
            pltpu.VMEM((1, BLK), i32), pltpu.SMEM((2, N_PAR), i32),
            pltpu.VMEM((BLK, WIDTH), f32), pltpu.VMEM((BLK, WIDTH), f32), pltpu.VMEM((BLK, BLK), jnp.bfloat16),
            pltpu.VMEM((6, BLK, WIDTH), jnp.bfloat16),
            pltpu.VMEM((N_DP, PAIR, WIDTH), f32), pltpu.VMEM((N_DP, PAIR, WIDTH), f32),
            pltpu.VMEM((N_PAR * NX, PAIR, WIDTH), f32),
            pltpu.VMEM((N_DP, 1, 128), i32), pltpu.VMEM((N_DP, 1, 128), i32),
            dma((4,)), dma, dma((N_DP,)), dma, dma, dma, dma((N_PAR,)), pltpu.SemaphoreType.REGULAR((3,)),
        ],
        compiler_params=pltpu.CompilerParams(collective_id=0, has_side_effects=True, vmem_limit_bytes=32 * 2**20),
    )(*(pltpu.with_memory_space_constraint(a, pltpu.HBM)
        for a in (first_moment, second_moment, new_owner.reshape(1, BLK), code_index)))
    return pl.pallas_call(
        put_out,
        out_shape=(jax.ShapeDtypeStruct((capacity, WIDTH), f32), jax.ShapeDtypeStruct((capacity, WIDTH), f32),
                   jax.ShapeDtypeStruct((capacity // N_PAR, 4 * WIDTH), f32), jax.ShapeDtypeStruct((1, 1), i32)),
        in_specs=[vmem, vmem, vmem, vmem],
        out_specs=(anywhere, anywhere, anywhere, anywhere),
        scratch_shapes=[pltpu.VMEM((1, 1), i32), pltpu.VMEM((capacity // N_PAR, 4 * WIDTH), f32),
                        dma((2 * PIECES + 1 + NX // 2,))],
        compiler_params=pltpu.CompilerParams(vmem_limit_bytes=16 * 2**20),
    )(*held)


def solution(mesh):
    rows = P(("dp", "parity"), None)
    return jax.shard_map(body, mesh=mesh, in_specs=(rows, rows, rows, P()),
                         out_specs=(rows, rows, rows, P("dp", "parity")), check_vma=False)
```
